128 devices in a mesh: rep: 1, r: 16 (over y, z), s: 8 (over x, core).
Axes of the slice: x: 4, y: 4, z: 4, core: 2. Of those that a mesh axis runs over, the one named last changes fastest.
Arguments:
- x: bfloat16 [128, 2048, 1280], P(('rep', 'r', 's'))
- dy: bfloat16 [128, 2048, 1280], P(('rep', 'r', 's'))
- w_gate: bfloat16 [2, 1280, 3584], P(None, 's')
- w_up: bfloat16 [2, 1280, 3584], P(None, 's')
- w_down: bfloat16 [2, 3584, 1280], P(None, 's')
- m_w_gate: float32 [2, 1280, 3584], P(None, 's')
- m_w_up: float32 [2, 1280, 3584], P(None, 's')
- m_w_down: float32 [2, 3584, 1280], P(None, 's')
- v_w_gate: float32 [2, 1280, 3584], P(None, 's')
- v_w_up: float32 [2, 1280, 3584], P(None, 's')
- v_w_down: float32 [2, 3584, 1280], P(None, 's')
Outputs:
- output 1: bfloat16 [2, 1280, 3584], P('rep', 's')
- output 2: bfloat16 [2, 1280, 3584], P('rep', 's')
- output 3: bfloat16 [2, 3584, 1280], P('rep', 's')
- output 4: float32 [2, 1280, 3584], P('rep', 's')
- output 5: float32 [2, 1280, 3584], P('rep', 's')
- output 6: float32 [2, 3584, 1280], P('rep', 's')
- output 7: float32 [2, 1280, 3584], P('rep', 's')
- output 8: float32 [2, 1280, 3584], P('rep', 's')
- output 9: float32 [2, 3584, 1280], P('rep', 's')
All inputs are finite; a program needn't handle non-finite values.
Results may differ from the reference program's by a relative error of at most 0.022.
Values are sent between devices in bfloat16 or wider.
A program may use at most 1.5 GiB of HBM per device.

```python
import jax
import jax.numpy as jnp
from jax import lax

SEQUENCES = 128
TOKENS = 2048
D = 1280
FF = 3584
LAYERS = 2
NAMES = ("w_gate", "w_up", "w_down")
SHAPES = {"w_gate": (LAYERS, D, FF), "w_up": (LAYERS, D, FF), "w_down": (LAYERS, FF, D)}


def bump(key, n, height):
    away = (jnp.arange(n, dtype=jnp.int32) - jax.random.randint(key, (), 0, n, jnp.int32)) % n
    return jnp.where(away < n // 8, height, 1.0)


def together(key, own, strength):
    shared = jax.random.normal(key, own.shape[1:], jnp.float32)
    return (own + strength * shared) * lax.rsqrt(1 + strength * strength)


def setup_inputs(seed: int = 0, part: int = 0) -> dict:
    kx, kdy, ka, kb, kz, kf, kh, kl, *keys = jax.random.split(jax.random.key(seed), 8 + 3 * len(NAMES))
    kx, kdy, ka, kb = (jax.random.fold_in(k, part) for k in (kx, kdy, ka, kb))
    kw, km, kv = (keys[i::3] for i in range(3))
    shape = (SEQUENCES, TOKENS, D)
    much_x, much_dy = jax.random.uniform(kz, (2,), jnp.float32, 0.0, 1.0)
    loud = 2.0 ** jax.random.uniform(jax.random.fold_in(kz, 1), (), jnp.float32, -1.0, 2.0)
    layers = 2.0 ** jax.random.uniform(kl, (LAYERS, 1, 1), jnp.float32, -1.0, 1.0)
    x = together(ka, jax.random.normal(kx, shape, jnp.float32), much_x) * bump(kf, D, 4.0)
    dy = together(kb, jax.random.normal(kdy, shape, jnp.float32), much_dy)
    drawn = {"x": x.astype(jnp.bfloat16), "dy": (loud * dy * (SEQUENCES * TOKENS) ** -0.5).astype(jnp.bfloat16)}
    for key, name in zip(kw, NAMES, strict=True):
        w = jax.random.normal(key, SHAPES[name], jnp.float32) * SHAPES[name][1] ** -0.5
        drawn[name] = (w * {"w_gate": 1.0, "w_up": bump(kh, FF, 4.0), "w_down": layers}[name]).astype(jnp.bfloat16)
    for key, name in zip(km, NAMES, strict=True):
        drawn[f"m_{name}"] = 0.1 * jax.random.normal(key, SHAPES[name], jnp.float32)
    for key, name in zip(kv, NAMES, strict=True):
        drawn[f"v_{name}"] = jax.random.uniform(key, SHAPES[name], jnp.float32, 0.005, 0.015)
    return drawn


def matmul(a, w):
    return jnp.dot(a, w, preferred_element_type=jnp.float32).astype(jnp.bfloat16)


def normed(h):
    wide = h.astype(jnp.float32)
    scale = lax.rsqrt(jnp.mean(wide**2, -1, keepdims=True) + 1e-6)
    return (wide * scale).astype(jnp.bfloat16)


def layer(h, w):
    a = normed(h)
    gate = jnp.dot(a, w["w_gate"], preferred_element_type=jnp.float32)
    up = jnp.dot(a, w["w_up"], preferred_element_type=jnp.float32)
    return h + matmul((jax.nn.silu(gate) * up).astype(jnp.bfloat16), w["w_down"])


def adamw(w, m, v, g):
    m = 0.9 * m + 0.1 * g
    v = 0.95 * v + 0.05 * g * g
    step = m * lax.rsqrt(v + 1e-8) + 0.1 * w
    return (w - 0.02 * step).astype(jnp.bfloat16), m, v


def clipped(gradients, sum_of_squares, count):
    factor = jnp.minimum(1.0, 0.5 * lax.rsqrt(sum_of_squares / count + 1e-30))
    return [g * factor for g in gradients]


def stack(weights, h):
    return lax.scan(lambda h, w: (layer(h, w), None), h, weights)[0]


def reference(x, dy, w_gate, w_up, w_down, m_w_gate, m_w_up, m_w_down, v_w_gate, v_w_up, v_w_down):
    weights = dict(zip(NAMES, (w_gate, w_up, w_down), strict=True))

    def take(so_far, sequence):
        h, by_y = sequence
        _, back = jax.vjp(lambda w: stack(w, h), weights)
        return jax.tree.map(lambda total, term: total + term.astype(jnp.float32), so_far, back(by_y)[0]), None

    none_yet = {name: jnp.zeros(w.shape, jnp.float32) for name, w in weights.items()}
    by_weights, _ = lax.scan(take, none_yet, (x, dy))
    gradients = [by_weights[name].astype(jnp.bfloat16).astype(jnp.float32) for name in NAMES]
    gradients = clipped(gradients, sum(jnp.sum(g * g) for g in gradients), sum(g.size for g in gradients))
    new = [
        adamw(w.astype(jnp.float32), m, v, g)
        for w, m, v, g in zip((w_gate, w_up, w_down), (m_w_gate, m_w_up, m_w_down), (v_w_gate, v_w_up, v_w_down), gradients, strict=True)
    ]
    return tuple(one[which] for which in range(3) for one in new)
```

```python
import functools

import jax
import jax.numpy as jnp
from jax import lax
from jax.experimental import pallas as pl
from jax.experimental.pallas import tpu as pltpu
from jax.sharding import PartitionSpec as P

bf16, f32 = jnp.bfloat16, jnp.float32
MESH = pl.DeviceIdType.MESH
VMEM_ALL = 67043328
ORDERS = ((0, 1, 2), (1, 2, 0), (2, 0, 1))


class Place:
    def __init__(self):
        rep, r, s = lax.axis_index("rep"), lax.axis_index("r"), lax.axis_index("s")
        self.rep = rep
        self.c = lax.rem(s, 2)
        self.at = (s // 2, r // 4, lax.rem(r, 4))

    def id(self, x, y, z, c):
        return (self.rep, y * 4 + z, x * 2 + c)

    def along(self, axis, k):
        at = list(self.at)
        at[axis] = lax.rem(at[axis] + k, 4)
        return at[axis], self.id(*at, self.c)

    def partner(self):
        return self.id(*self.at, 1 - self.c)

    def meet(self, more=()):
        barrier = pltpu.get_barrier_semaphore()
        ids = [self.partner()] + [self.along(a, k)[1] for a in range(3) for k in (1, 2, 3)] + list(more)
        for i in ids:
            pl.semaphore_signal(barrier, inc=1, device_id=i, device_id_type=MESH)
        pl.semaphore_wait(barrier, len(ids))


def arrive(ref, sem):
    pltpu.make_async_copy(ref, ref, sem).wait()


def send(src, dst, send_sem, recv_sem, to):
    pltpu.make_async_remote_copy(src_ref=src, dst_ref=dst, send_sem=send_sem, recv_sem=recv_sem, device_id=to, device_id_type=MESH).start()


class Sum:
    def __init__(self, units, rows, cols, parts, ring=None):
        self.units, self.rows, self.cols, self.parts = units, rows, cols, parts
        self.sizes = [(p[0][1], p[1][1]) for p in parts]

    def scratch(self):
        u = self.units
        shapes = dict(s=pltpu.VMEM((u, 4, 4, 4, self.rows, self.cols), bf16), ga=pltpu.VMEM((u, 4, 4, self.rows, self.cols), bf16))
        for k, (r, c) in enumerate(self.sizes):
            shapes[f"p1{k}"] = pltpu.VMEM((u, 3, 4, 4, r, c), bf16)
            shapes[f"o1{k}"] = pltpu.VMEM((u, 4, 4, r, c), f32)
            shapes[f"p2{k}"] = pltpu.VMEM((u, 3, 4, r, c), bf16)
            shapes[f"o2{k}"] = pltpu.VMEM((u, 4, r, c), f32)
            shapes[f"p3{k}"] = pltpu.VMEM((u, 3, r, c), bf16)
        shapes["snd"] = pltpu.SemaphoreType.DMA((5, u, 3))
        shapes["rcv"] = pltpu.SemaphoreType.DMA((5, u, 3))
        return shapes

    def bind(self, place, refs):
        self.place, self.ref = place, refs
        return self

    def cut(self, k):
        (r0, r), (c0, c) = self.parts[k]
        return pl.ds(r0, r), pl.ds(c0, c)

    def own(self, k):
        return self.place.at[ORDERS[k][0]]

    def piece(self, k, q):
        axis = ORDERS[k][0]
        return tuple(q if a == axis else slice(None) for a in range(3))

    def start1(self, u):
        R = self.ref
        for k in range(3):
            for j in (1, 2, 3):
                q, to = self.place.along(ORDERS[k][0], j)
                send(R["s"].at[(u,) + self.piece(k, q) + self.cut(k)], R[f"p1{k}"].at[u, j - 1], R["snd"].at[0, u, k], R["rcv"].at[0, u, k], to)

    def add1(self, u):
        R = self.ref
        for k in range(3):
            p, o = R[f"p1{k}"], R[f"o1{k}"]
            arrive(p.at[u], R["rcv"].at[0, u, k])

            def some(i, _, p=p, o=o):
                t = o[u, i] + p[u, 0, i].astype(f32) + p[u, 1, i].astype(f32) + p[u, 2, i].astype(f32)
                o[u, i] = t
                p[u, 0, i] = t.astype(bf16)
                return 0

            lax.fori_loop(0, 4, some, 0)
            axis = ORDERS[k][1]
            for j in (1, 2, 3):
                q, to = self.place.along(axis, j)
                at = (u, 0, q) if self.second_is_first(k) else (u, 0, slice(None), q)
                send(p.at[at], R[f"p2{k}"].at[u, j - 1], R["snd"].at[1, u, k], R["rcv"].at[1, u, k], to)

    def second_is_first(self, k):
        left = [a for a in range(3) if a != ORDERS[k][0]]
        return left[0] == ORDERS[k][1]

    def add2(self, u):
        R = self.ref
        for k in range(3):
            p, o1, o = R[f"p2{k}"], R[f"o1{k}"], R[f"o2{k}"]
            arrive(p.at[u], R["rcv"].at[1, u, k])
            me = self.place.at[ORDERS[k][1]]
            for i in range(4):
                mine = o1[u, me, i] if self.second_is_first(k) else o1[u, i, me]
                t = mine + p[u, 0, i].astype(f32) + p[u, 1, i].astype(f32) + p[u, 2, i].astype(f32)
                o[u, i] = t
                p[u, 0, i] = t.astype(bf16)
            for j in (1, 2, 3):
                q, to = self.place.along(ORDERS[k][2], j)
                send(p.at[u, 0, q], R[f"p3{k}"].at[u, j - 1], R["snd"].at[2, u, k], R["rcv"].at[2, u, k], to)

    def first(self, k):
        return 1 if k != 1 else 2

    def add3(self, u):
        R = self.ref
        _, y, z = self.place.at
        for k in range(3):
            p, o = R[f"p3{k}"], R[f"o2{k}"]
            arrive(p.at[u], R["rcv"].at[2, u, k])
            t = o[u, self.place.at[ORDERS[k][2]]] + p[u, 0].astype(f32) + p[u, 1].astype(f32) + p[u, 2].astype(f32)
            (r0, r), (c0, c) = self.parts[k]
            R["ga"][u, y, z, r0 : r0 + r, c0 : c0 + c] = t.astype(bf16)
            mine = R["ga"].at[(u, y, z) + self.cut(k)]
            for j in (1, 2, 3):
                _, to = self.place.along(self.first(k), j)
                send(mine, mine, R["snd"].at[3, u, k], R["rcv"].at[3, u, k], to)

    def gather(self, u):
        R = self.ref
        _, y, z = self.place.at
        for k in range(3):
            arrive(R["ga"].at[(u, pl.ds(0, 3), 0) + self.cut(k)], R["rcv"].at[3, u, k])
            at = (u, slice(None), z) if self.first(k) == 1 else (u, y, slice(None))
            line = R["ga"].at[at + self.cut(k)]
            for j in (1, 2, 3):
                _, to = self.place.along(3 - self.first(k), j)
                send(line, line, R["snd"].at[4, u, k], R["rcv"].at[4, u, k], to)

    def gathered(self, u):
        R = self.ref
        for k in range(3):
            arrive(R["ga"].at[(u, pl.ds(0, 3), slice(None)) + self.cut(k)], R["rcv"].at[4, u, k])

    def finish(self):
        R = self.ref

        def one(u, _):
            for k in range(3):
                arrive(R[f"p1{k}"].at[u], R["snd"].at[0, u, k])
                arrive(R[f"p2{k}"].at[u], R["snd"].at[1, u, k])
                arrive(R[f"p3{k}"].at[u], R["snd"].at[2, u, k])
                arrive(R["ga"].at[(u, pl.ds(0, 3), 0) + self.cut(k)], R["snd"].at[3, u, k])
                arrive(R["ga"].at[(u, pl.ds(0, 3), slice(None)) + self.cut(k)], R["snd"].at[4, u, k])
            return 0

        lax.fori_loop(0, self.units, one, 0)

    def stages(self, t):
        for lag, stage in ((2, self.add1), (3, self.add2), (4, self.add3), (5, self.gather), (6, self.gathered)):
            u = t - lag

            @pl.when((u >= 0) & (u < self.units))
            def _(stage=stage, u=u):
                stage(u)


GU = Sum(7, 80, 128, (((0, 32), (0, 128)), ((32, 32), (0, 128)), ((64, 16), (0, 128))))
DOWN = Sum(1, 56, 640, (((0, 56), (0, 256)), ((0, 56), (256, 256)), ((0, 56), (512, 128))))


def own_parts(rs, u, oh, x=None):
    R = rs.ref
    for k in range(3):
        me = rs.own(k)
        (r0, r), (c0, c) = rs.parts[k]
        for i in range(4):
            for j in range(4):
                rest = [i, j]
                at = tuple(me if a == ORDERS[k][0] else rest.pop(0) for a in range(3))
                yield k, i, j, at, (slice(r0, r0 + r), slice(c0, c0 + c))


def gu_halves(rs, u, slot, oh, d2d):
    R = rs.ref
    arrive(R["s"].at[u], d2d.at[u])
    for k in range(3):
        me = rs.own(k)
        (r0, r), (c0, c) = rs.parts[k]

        def some(i, _, k=k, me=me, r0=r0, r=r):
            for j in range(4):
                rest = [i, j]
                at = tuple(me if a == ORDERS[k][0] else rest.pop(0) for a in range(3))
                R[f"o1{k}"][u, i, j] = oh[(slot,) + at + (slice(r0, r0 + r),)] + R["s"][(u,) + at + (slice(r0, r0 + r),)].astype(f32)
            return 0

        lax.fori_loop(0, 4, some, 0)

    def all_of(i, _):
        x, y = i // 4, lax.rem(i, 4)
        for z in range(4):
            R["s"][u, x, y, z] = (oh[slot, x, y, z] + R["s"][u, x, y, z].astype(f32)).astype(bf16)
        return 0

    lax.fori_loop(0, 16, all_of, 0)
    rs.start1(u)


def gu_kernel(aT, dg, du, ga_out, *scratch, names):
    refs = dict(zip(names, scratch, strict=True))
    place = Place()
    c = place.c
    rs = GU.bind(place, refs)
    a, r, oh, sb, asem, rsem, d2d_s, d2d_r, osem = (refs[n] for n in ("a", "r", "oh", "sb", "asem", "rsem", "d2d_s", "d2d_r", "osem"))

    def chunk(m, j, slot):
        src = (dg, du)[m]
        return pltpu.make_async_copy(src.at[:, pl.ds(pl.multiple_of(j * 512, 512), 512)], r.at[slot, m], rsem.at[slot, m])

    for h in range(2):
        pltpu.make_async_copy(aT.at[:, 1 - c if h == 0 else c], a.at[h], asem.at[h]).start()
    for m in range(2):
        chunk(m, 0, 0).start()
    place.meet()
    for h in range(2):
        arrive(a.at[h], asem.at[h])

    def step(t, _):
        slot = lax.rem(t, 2)

        @pl.when(t < 7)
        def _():
            @pl.when(t + 1 < 7)
            def _():
                for m in range(2):
                    chunk(m, t + 1, 1 - slot).start()

            @pl.when(t >= 2)
            def _():
                arrive(sb.at[slot], d2d_s.at[slot])

            for m in range(2):
                chunk(m, t, slot).wait()
                res = jnp.dot(a[...].reshape(1280, 2048), r[slot, m], preferred_element_type=f32)
                for x in range(4):
                    for h in range(2):
                        for y in range(4):
                            row = x * 160 + h * 80
                            sb[slot, x, y, 2 * m + h] = res[row : row + 80, y * 128 : y * 128 + 128].astype(bf16)
                            oh[slot, x, y, 2 * m + h] = res[640 + row : 640 + row + 80, y * 128 : y * 128 + 128]
            send(sb.at[slot], refs["s"].at[t], d2d_s.at[slot], d2d_r.at[t], place.partner())

        @pl.when((t >= 1) & (t < 8))
        def _():
            gu_halves(rs, t - 1, 1 - slot, oh, d2d_r)

        rs.stages(t)
        return 0

    lax.fori_loop(0, 13, step, 0)
    for slot in range(2):
        arrive(sb.at[slot], d2d_s.at[slot])
    rs.finish()
    out = pltpu.make_async_copy(refs["ga"], ga_out, osem)
    out.start()
    out.wait()


def gu_grads(aT, dg, du, collective_id):
    scratch = GU.scratch()
    scratch.update(
        a=pltpu.VMEM((2, 4, 160, 2048), bf16),
        r=pltpu.VMEM((2, 2, 2048, 512), bf16),
        oh=pltpu.VMEM((2, 4, 4, 4, 80, 128), f32),
        sb=pltpu.VMEM((2, 4, 4, 4, 80, 128), bf16),
        asem=pltpu.SemaphoreType.DMA((2,)),
        rsem=pltpu.SemaphoreType.DMA((2, 2)),
        d2d_s=pltpu.SemaphoreType.DMA((2,)),
        d2d_r=pltpu.SemaphoreType.DMA((7,)),
        osem=pltpu.SemaphoreType.DMA,
    )
    out = pl.pallas_call(
        functools.partial(gu_kernel, names=tuple(scratch)),
        out_shape=jax.ShapeDtypeStruct((7, 4, 4, 80, 128), bf16),
        in_specs=[pl.BlockSpec(memory_space=pl.ANY)] * 3,
        out_specs=pl.BlockSpec(memory_space=pl.ANY),
        scratch_shapes=list(scratch.values()),
        compiler_params=pltpu.CompilerParams(collective_id=collective_id, has_side_effects=True, vmem_limit_bytes=VMEM_ALL),
        name="gu_grads",
    )(aT.reshape(4, 2, 160, 2048), dg, du)
    out = out.reshape(7, 4, 2, 2, 80, 128).transpose(2, 3, 4, 0, 1, 5).reshape(2, 160, 3584)
    return out[0], out[1]


def down_half(rs, x, slot, oh, d2d):
    R = rs.ref
    arrive(R["s"].at[0, x], d2d.at[x])
    xm, ym, zm = rs.place.at
    s, (c0, c1, c2) = R["s"], [slice(p[1][0], p[1][0] + p[1][1]) for p in rs.parts]
    for i in range(4):
        R["o11"][0, x, i] = oh[slot, ym, i, :, c1] + s[0, x, ym, i, :, c1].astype(f32)
        R["o12"][0, x, i] = oh[slot, i, zm, :, c2] + s[0, x, i, zm, :, c2].astype(f32)

    @pl.when(x == xm)
    def _():
        for i in range(4):
            for j in range(4):
                R["o10"][0, i, j] = oh[slot, i, j, :, c0] + s[0, x, i, j, :, c0].astype(f32)

    def all_of(y, _):
        for z in range(4):
            s[0, x, y, z] = (oh[slot, y, z] + s[0, x, y, z].astype(f32)).astype(bf16)
        return 0

    lax.fori_loop(0, 4, all_of, 0)


def down_kernel(hid, dy, ga_out, *scratch, names):
    refs = dict(zip(names, scratch, strict=True))
    place = Place()
    rs = DOWN.bind(place, refs)
    l, d, t_ref, oh, sb, lsem, dsem, d2d_s, d2d_r, osem = (refs[n] for n in ("l", "d", "t", "oh", "sb", "lsem", "dsem", "d2d_s", "d2d_r", "osem"))

    def chunk(x, slot):
        return pltpu.make_async_copy(hid.at[:, pl.ds(pl.multiple_of(x * 896, 128), 896)], l.at[slot], lsem.at[slot])

    whole = pltpu.make_async_copy(dy, d, dsem)
    whole.start()
    chunk(0, 0).start()
    place.meet()
    whole.wait()

    def step(x, _):
        slot = lax.rem(x, 2)

        @pl.when(x < 4)
        def _():
            @pl.when(x + 1 < 4)
            def _():
                chunk(x + 1, 1 - slot).start()

            @pl.when(x >= 2)
            def _():
                arrive(sb.at[slot], d2d_s.at[slot])

            chunk(x, slot).wait()
            t_ref[...] = lax.dot_general(l[slot], d[...], (((0,), (0,)), ((), ())), preferred_element_type=f32).reshape(2, 448, 1280)
            for y in range(4):
                for z in range(4):
                    row, col = y * 112 + (z // 2) * 56, (z % 2) * 640
                    sb[slot, y, z] = t_ref[1 - place.c, row : row + 56, col : col + 640].astype(bf16)
                    oh[slot, y, z] = t_ref[place.c, row : row + 56, col : col + 640]
            send(sb.at[slot], refs["s"].at[0, x], d2d_s.at[slot], d2d_r.at[x], place.partner())

        @pl.when(x >= 1)
        def _():
            down_half(rs, x - 1, 1 - slot, oh, d2d_r)

        return 0

    lax.fori_loop(0, 5, step, 0)
    rs.start1(0)
    rs.add1(0)
    rs.add2(0)
    rs.add3(0)
    rs.gather(0)
    rs.gathered(0)
    for slot in range(2):
        arrive(sb.at[slot], d2d_s.at[slot])
    rs.finish()
    out = pltpu.make_async_copy(refs["ga"], ga_out, osem)
    out.start()
    out.wait()


def down_grads(hid, dy, collective_id):
    scratch = DOWN.scratch()
    scratch.update(
        l=pltpu.VMEM((2, 2048, 896), bf16),
        d=pltpu.VMEM((2048, 1280), bf16),
        t=pltpu.VMEM((2, 448, 1280), f32),
        oh=pltpu.VMEM((2, 4, 4, 56, 640), f32),
        sb=pltpu.VMEM((2, 4, 4, 56, 640), bf16),
        lsem=pltpu.SemaphoreType.DMA((2,)),
        dsem=pltpu.SemaphoreType.DMA,
        d2d_s=pltpu.SemaphoreType.DMA((2,)),
        d2d_r=pltpu.SemaphoreType.DMA((4,)),
        osem=pltpu.SemaphoreType.DMA,
    )
    out = pl.pallas_call(
        functools.partial(down_kernel, names=tuple(scratch)),
        out_shape=jax.ShapeDtypeStruct((1, 4, 4, 56, 640), bf16),
        in_specs=[pl.BlockSpec(memory_space=pl.ANY)] * 2,
        out_specs=pl.BlockSpec(memory_space=pl.ANY),
        scratch_shapes=list(scratch.values()),
        compiler_params=pltpu.CompilerParams(collective_id=collective_id, has_side_effects=True, vmem_limit_bytes=VMEM_ALL),
        name="down_grads",
    )(hid, dy)
    return out.reshape(4, 2, 2, 56, 640).transpose(0, 1, 3, 2, 4).reshape(448, 1280)
NAMES = ("w_gate", "w_up", "w_down")


def matmul(a, w):
    return jnp.dot(a, w, preferred_element_type=f32).astype(bf16)


def scale_of(h):
    wide = h.astype(f32)
    return lax.rsqrt(jnp.mean(wide**2, -1, keepdims=True) + 1e-6)


def normed(h, scale):
    return (h.astype(f32) * scale).astype(bf16)


def adamw(w, m, v, g):
    m = 0.9 * m + 0.1 * g
    v = 0.95 * v + 0.05 * g * g
    step = m * lax.rsqrt(v + 1e-8) + 0.1 * w
    return (w - 0.02 * step).astype(bf16), m, v


def clipped(gradients, sum_of_squares, count):
    factor = jnp.minimum(1.0, 0.5 * lax.rsqrt(sum_of_squares / count + 1e-30))
    return [g * factor for g in gradients]


def back_norm(by_a, h, scale):
    by_a, wide = by_a.astype(f32), h.astype(f32)
    along = jnp.mean(by_a * wide, -1, keepdims=True)
    return (by_a * scale - wide * (scale**3 * along)).astype(bf16)


def solution(mesh):
    def fetched(weights, number):
        return [lax.all_gather(w[number], "s", axis=0, tiled=True) for w in weights]

    def step(x, dy, *arrays):
        weights, m, v = (arrays[i : i + 3] for i in (0, 3, 6))
        h, by_y, kept = x[0], dy[0], []
        for number in range(2):
            w_gate, w_up, w_down = fetched(weights, number)
            scale = scale_of(h)
            a = normed(h, scale)
            gate, up = (jnp.dot(a, w, preferred_element_type=f32) for w in (w_gate, w_up))
            hid = (jax.nn.silu(gate) * up).astype(bf16)
            kept.append((h, scale, a, gate, up, hid, w_gate, w_up, w_down))
            h = h + matmul(hid, w_down)
        mine = [None, None]
        for number in (1, 0):
            h, scale, a, gate, up, hid, w_gate, w_up, w_down = kept[number]
            by_hid = matmul(by_y, w_down.T).astype(f32)
            sig = jax.nn.sigmoid(gate)
            by_up = (by_hid * (gate * sig)).astype(bf16)
            by_gate = (by_hid * up * (sig * (1.0 + gate * (1.0 - sig)))).astype(bf16)
            down = down_grads(hid, by_y, 2 * number)
            g, u = gu_grads(a.T, by_gate, by_up, 2 * number + 1)
            mine[number] = (g, u, down)
            if number:
                by_a = matmul(by_gate, w_gate.T) + matmul(by_up, w_up.T)
                by_y = by_y + back_norm(by_a, h, scale)
        gradients = [jnp.stack([mine[number][i] for number in range(2)]).astype(f32) for i in range(3)]
        squares = lax.psum(sum(jnp.sum(g * g) for g in gradients), "s")
        gradients = clipped(gradients, squares, 8 * sum(g.size for g in gradients))
        new = [adamw(w.astype(f32), m, v, g) for w, m, v, g in zip(weights, m, v, gradients, strict=True)]
        return tuple(one[which] for which in range(3) for one in new)

    states, cut = P(("rep", "r", "s"), None, None), P(None, "s", None)
    return jax.shard_map(
        step,
        mesh=mesh,
        in_specs=(states, states) + (cut,) * 9,
        out_specs=(P("rep", "s", None),) * 9,
        check_vma=False,
    )
```

```python
import functools

import jax
import jax.numpy as jnp
from jax import lax
from jax.experimental import pallas as pl
from jax.experimental.pallas import tpu as pltpu
from jax.sharding import PartitionSpec as P

bf16, f32 = jnp.bfloat16, jnp.float32
MESH = pl.DeviceIdType.MESH
VMEM_ALL = 67043328
T, D, F, LAYERS = 2048, 1280, 3584, 2
CORES, RING, LANES = 2, 4, 128
BLOCKS = RING * CORES
N, TILE = 512, 1024
CHUNKS = F // N
ROWS, ROWS_DOWN = D // BLOCKS, F // BLOCKS
WIDE = F // RING
X, Y, Z = range(3)
AXES = (X, Y, Z)
ORDERS = ((X, Y, Z), (Y, Z, X), (Z, X, Y))
OTHERS = (1, 3, 2)
ALL = slice(None)
ROW_BY_ROW, BY_LAST = (((0,), (0,)), ((), ())), (((1,), (1,)), ((), ()))


def at(i, n):
    return pl.ds(pl.multiple_of(i * n, n), n)


def sem(*shape):
    return pltpu.SemaphoreType.DMA(shape)


def loop(n, body):
    def step(i, none):
        body(i)
        return none

    lax.fori_loop(0, n, step, 0)


def when(condition, do, *args):
    pl.when(condition)(functools.partial(do, *args))


def within(t, n, stage):
    when((t >= 0) & (t < n), stage, t)


def start(copies):
    for copy in copies:
        copy.start()


def wait(copies):
    for copy in copies:
        copy.wait()


def arrive(ref, semaphore):
    pltpu.make_async_copy(ref, ref, semaphore).wait()


def send(src, dst, sent, come, to):
    pltpu.make_async_remote_copy(src_ref=src, dst_ref=dst, send_sem=sent, recv_sem=come, device_id=to, device_id_type=MESH).start()


class Place:
    def __init__(self):
        r, s = lax.axis_index("r"), lax.axis_index("s")
        self.rep = lax.axis_index("rep")
        self.core = lax.rem(s, CORES)
        self.at = (s // CORES, r // RING, lax.rem(r, RING))

    def id(self, x, y, z, core):
        return (self.rep, y * RING + z, x * CORES + core)

    def along(self, axis, k):
        there = list(self.at)
        there[axis] = lax.rem(there[axis] + k, RING)
        return there[axis], self.id(*there, self.core)

    def partner(self):
        return self.id(*self.at, 1 - self.core)

    def shard_group(self):
        x, y, z = self.at
        return [self.id(lax.rem(x + k, RING), y, z, 1 - self.core) for k in OTHERS]

    def meet(self, more=()):
        barrier = pltpu.get_barrier_semaphore()
        ids = [self.partner()] + [self.along(a, k)[1] for a in AXES for k in OTHERS] + list(more)
        for i in ids:
            pl.semaphore_signal(barrier, device_id=i, device_id_type=MESH)
        pl.semaphore_wait(barrier, len(ids))


class Gather:
    ALONE, QUARTER = 32, 16

    @staticmethod
    def scratch():
        return dict(g_own=sem(CHUNKS), g_snd=sem(3, CHUNKS), g_rcv=sem(3, CHUNKS))

    def __init__(self, place, refs, w, sources, layer, blocks=None):
        self.place, self.w, self.sources, self.layer, self.blocks = place, w, sources, layer, blocks
        self.own, self.snd, self.rcv = refs["g_own"], refs["g_snd"], refs["g_rcv"]
        _, y, z = place.at
        self.parts = [pl.ds(pl.multiple_of(self.ALONE + self.QUARTER * i, self.QUARTER), self.QUARTER) for i in (y, RING + z)]

    def some(self, j, parts, semaphores, stage):
        arrive(self.w.at[j, :, pl.ds(0, 3), 0, pl.ds(0, parts)], semaphores.at[stage, j])

    def start_x(self, j):
        mine = self.w.at[j, :, self.place.at[X], self.place.core]
        for m, source in enumerate(self.sources):
            for k in OTHERS:
                _, to = self.place.along(X, k)
                for rows in [pl.ds(0, self.ALONE)] + self.parts:
                    send(source.at[self.layer, rows, at(j, N)], mine.at[m, rows], self.snd.at[X, j], self.rcv.at[X, j], to)
            block = source.at[self.layer] if self.blocks is None else self.blocks.at[m]
            pltpu.make_async_copy(block.at[:, at(j, N)], mine.at[m], self.own.at[j]).start()

    def start_yz(self, j):
        self.some(j, self.ALONE + 2 * self.QUARTER, self.rcv, X)
        for k in OTHERS:
            for axis, rows in zip((Y, Z), self.parts, strict=True):
                _, to = self.place.along(axis, k)
                for i in OTHERS:
                    part = self.w.at[j, :, self.place.along(X, i)[0], self.place.core, rows]
                    send(part, part, self.snd.at[Y, j], self.rcv.at[Y, j], to)

    def start_d(self, j):
        self.some(j, 2 * 3 * self.QUARTER, self.rcv, Y)
        arrive(self.w.at[j, :, 0, 0], self.own.at[j])
        half = self.w.at[j, :, :, self.place.core]
        send(half, half, self.snd.at[Z, j], self.rcv.at[Z, j], self.place.partner())

    def ready(self, j):
        arrive(self.w.at[j, :, :, 0], self.rcv.at[Z, j])

    def finish(self):
        def one(j):
            self.some(j, self.ALONE + 2 * self.QUARTER, self.snd, X)
            self.some(j, 2 * 3 * self.QUARTER, self.snd, Y)
            arrive(self.w.at[j, :, :, 0], self.snd.at[Z, j])

        loop(CHUNKS, one)


class DownGather:
    UNITS = 5
    ALONE, QUARTER = 64, 48

    @classmethod
    def scratch(cls):
        return dict(block=pltpu.VMEM((ROWS_DOWN, D), bf16), d_own=sem(2), d_snd=sem(3, cls.UNITS), d_rcv=sem(3, cls.UNITS))

    def __init__(self, place, refs, d, source, layer):
        self.place, self.d, self.source = place, d, source.at[layer]
        self.block, self.snd, self.rcv = refs["block"], refs["d_snd"], refs["d_rcv"]
        mine = d.at[place.at[X], place.core]
        self.load, self.store = (
            pltpu.make_async_copy(a, b, refs["d_own"].at[i]) for i, (a, b) in enumerate(((self.source, self.block), (self.block, mine)))
        )
        _, y, z = place.at
        self.parts = [pl.ds(pl.multiple_of(self.ALONE + self.QUARTER * i, 16), self.QUARTER) for i in (y, RING + z)]

    def columns(self, u):
        return at(u, D // self.UNITS)

    def some(self, u, parts, semaphores, stage):
        arrive(self.d.at[pl.ds(0, 3), 0, pl.ds(0, parts), pl.ds(0, D // self.UNITS)], semaphores.at[stage, u])

    def whole(self, u, semaphores):
        arrive(self.d.at[:, 0, :, pl.ds(0, D // self.UNITS)], semaphores.at[Z, u])

    def start_x(self, u):
        for k in OTHERS:
            _, to = self.place.along(X, k)
            for rows in [pl.ds(0, self.ALONE)] + self.parts:
                there = self.d.at[self.place.at[X], self.place.core, rows, self.columns(u)]
                send(self.source.at[rows, self.columns(u)], there, self.snd.at[X, u], self.rcv.at[X, u], to)

    def start_yz(self, u):
        self.some(u, self.ALONE + 2 * self.QUARTER, self.rcv, X)
        for k in OTHERS:
            for axis, rows in zip((Y, Z), self.parts, strict=True):
                _, to = self.place.along(axis, k)
                for i in OTHERS:
                    part = self.d.at[self.place.along(X, i)[0], self.place.core, rows, self.columns(u)]
                    send(part, part, self.snd.at[Y, u], self.rcv.at[Y, u], to)

    def start_d(self, u):
        self.some(u, 2 * 3 * self.QUARTER, self.rcv, Y)
        mine = self.d.at[self.place.at[X], self.place.core, :, self.columns(u)]
        pairs = [(self.source.at[:, self.columns(u)], mine)]
        for i in OTHERS:
            pairs.append((self.d.at[self.place.along(X, i)[0], self.place.core, :, self.columns(u)],) * 2)
        for src, dst in pairs:
            send(src, dst, self.snd.at[Z, u], self.rcv.at[Z, u], self.place.partner())

    def ready(self, u):
        self.whole(u, self.rcv)

    def finish(self):
        self.load.wait()
        self.store.start()
        loop(self.UNITS, self.ready)

        def one(u):
            self.some(u, self.ALONE + 2 * self.QUARTER, self.snd, X)
            self.some(u, 2 * 3 * self.QUARTER, self.snd, Y)
            self.whole(u, self.snd)

        loop(self.UNITS, one)
        self.store.wait()


class Sum:
    def __init__(self, name, units, rows, cols, cuts, owns=1):
        self.name, self.units, self.rows, self.cols, self.cuts, self.owns = name, units, rows, cols, cuts, owns

    def scratch(self):
        u, piece = self.units, (self.rows, self.cols)
        shapes = dict(s=pltpu.VMEM((u, RING, RING, RING) + piece, bf16), ga=pltpu.VMEM((u, RING, RING) + piece, bf16))
        for k, (r, c) in enumerate(self.cuts):
            part = (r.stop - r.start, c.stop - c.start)
            shapes[f"own{k}"] = pltpu.VMEM((self.owns, RING, RING) + part, f32)
            if self.owns < u:
                shapes[f"one{k}"] = pltpu.VMEM((RING, RING) + part, f32)
            shapes[f"two{k}"] = pltpu.VMEM((RING,) + part, f32)
            shapes[f"p{k}"] = pltpu.VMEM((u, 3, RING, RING) + part, bf16)
            shapes[f"q{k}"] = pltpu.VMEM((u, 3, RING) + part, bf16)
            shapes[f"r{k}"] = pltpu.VMEM((u, 3) + part, bf16)
        shapes.update(snd=sem(5, u, 3), rcv=sem(5, u, 3))
        return {self.name + key: value for key, value in shapes.items()}

    def bind(self, place, refs, s=None):
        self.place = place
        self.ref = {key[len(self.name) :]: ref for key, ref in refs.items() if key.startswith(self.name)}
        self.s, self.ga = self.ref["s"] if s is None else s, self.ref["ga"]
        return self

    def refs(self, *names):
        return [(k, [self.ref[f"{name}{k}"] for name in names]) for k in AXES]

    def ones(self, k, u):
        return self.ref[f"one{k}"] if self.owns < self.units else self.ref[f"own{k}"].at[u]

    def piece(self, k, q, *rest):
        rest = list(rest) or [ALL, ALL]
        return tuple(q if a == ORDERS[k][0] else rest.pop(0) for a in AXES)

    def sem(self, name, stage, u, k):
        return self.ref[name].at[stage, u, k]

    def pass_on(self, stage, u, k, axis, pair):
        for n in OTHERS:
            q, to = self.place.along(axis, n)
            send(*pair(q, n - 1), self.sem("snd", stage, u, k), self.sem("rcv", stage, u, k), to)

    def start1(self, u):
        for k, (p,) in self.refs("p"):
            self.pass_on(0, u, k, ORDERS[k][0], lambda q, n, k=k, p=p: (self.s.at[(u,) + self.piece(k, q) + self.cuts[k]], p.at[u, n]))

    def leading(self, k):
        return ORDERS[k][1] < ORDERS[k][2]

    def add1(self, u):
        for k, (p, q, own) in self.refs("p", "q", "own"):
            one = self.ones(k, u)
            arrive(p.at[u], self.sem("rcv", 0, u, k))

            def some(i, p=p, own=own, one=one):
                t = own[lax.rem(u, self.owns), i] + p[u, 0, i].astype(f32) + p[u, 1, i].astype(f32) + p[u, 2, i].astype(f32)
                one[i] = t
                p[u, 0, i] = t.astype(bf16)

            loop(RING, some)
            self.pass_on(1, u, k, ORDERS[k][1], lambda i, n, k=k, p=p, q=q: (p.at[(u, 0, i) if self.leading(k) else (u, 0, ALL, i)], q.at[u, n]))

    def add2(self, u):
        for k, (q, r, two) in self.refs("q", "r", "two"):
            one = self.ones(k, u)
            arrive(q.at[u], self.sem("rcv", 1, u, k))
            me = self.place.at[ORDERS[k][1]]
            for i in range(RING):
                mine = one[me, i] if self.leading(k) else one[i, me]
                t = mine + q[u, 0, i].astype(f32) + q[u, 1, i].astype(f32) + q[u, 2, i].astype(f32)
                two[i] = t
                q[u, 0, i] = t.astype(bf16)
            self.pass_on(2, u, k, ORDERS[k][2], lambda i, n, q=q, r=r: (q.at[u, 0, i], r.at[u, n]))

    def lines(self, u, k):
        _, y, z = self.place.at
        return [self.ga.at[(u, y, to) + self.cuts[k]] for to in (z, ALL)]

    def add3(self, u):
        _, y, z = self.place.at
        for k, (r, two) in self.refs("r", "two"):
            arrive(r.at[u], self.sem("rcv", 2, u, k))
            t = two[self.place.at[ORDERS[k][2]]] + r[u, 0].astype(f32) + r[u, 1].astype(f32) + r[u, 2].astype(f32)
            self.ga[(u, y, z) + self.cuts[k]] = t.astype(bf16)
            mine, _ = self.lines(u, k)
            self.pass_on(3, u, k, Z, lambda q, n, mine=mine: (mine, mine))

    def three(self, u, k, name, stage):
        at = (u, pl.ds(0, 3), 0) if stage == 3 else (u, pl.ds(0, 3), ALL)
        arrive(self.ga.at[at + self.cuts[k]], self.sem(name, stage, u, k))

    def gather(self, u):
        for k in AXES:
            self.three(u, k, "rcv", 3)
            _, line = self.lines(u, k)
            self.pass_on(4, u, k, Y, lambda q, n, line=line: (line, line))

    def gathered(self, u):
        for k in AXES:
            self.three(u, k, "rcv", 4)

    def finish(self):
        def one(u):
            for k, parts in self.refs("p", "q", "r"):
                for stage, part in enumerate(parts):
                    arrive(part.at[u], self.sem("snd", stage, u, k))
                for stage in (3, 4):
                    self.three(u, k, "snd", stage)

        loop(self.units, one)

    def stages(self, t):
        for lag, stage in enumerate((self.gathered, self.gather, self.add3, self.add2, self.add1)):
            within(t + lag - 5, self.units, stage)


def whole(n):
    return slice(0, n)


THIRDS = tuple((slice(a, b), whole(LANES)) for a, b in ((0, 32), (32, 48), (48, 80)))
DOWN = Sum("low_", 1, 56, D // 2, tuple((whole(56), slice(a, b)) for a, b in ((0, 256), (256, 384), (384, 640))))


def gate_up_sum(name, units, owns=1):
    return Sum(name, units, ROWS // 2, LANES, THIRDS, owns)


class GateUp:
    @staticmethod
    def scratch():
        pieces = (RING, RING, RING, ROWS // 2, LANES)
        return dict(t=pltpu.VMEM((RING, CORES, ROWS, N), f32), oh=pltpu.VMEM(pieces, f32), sb=pltpu.VMEM(pieces, bf16), halfsem=sem())

    def __init__(self, place, refs, s, come):
        self.place, self.s, self.come = place, s, come
        self.t, self.oh, self.sb, self.sent = refs["t"], refs["oh"], refs["sb"], refs["halfsem"]

    def multiply(self, u, a, sides, free=None):
        for m, side in enumerate(sides):
            self.t[...] = lax.dot_general(a[...], side[...], ROW_BY_ROW, preferred_element_type=f32).reshape(self.t.shape)
            if not m:
                when(u > 0, arrive, self.sb, self.sent)
                if free:
                    free()

            def halve(x, m=m):
                for y in range(RING):
                    for h in range(2):
                        part = (slice(h * ROWS // 2, (h + 1) * ROWS // 2), slice(y * LANES, (y + 1) * LANES))
                        self.sb[x, y, 2 * m + h] = self.t[(x, 1 - self.place.core) + part].astype(bf16)
                        self.oh[x, y, 2 * m + h] = self.t[(x, self.place.core) + part]

            loop(RING, halve)
        send(self.sb, self.s.at[u], self.sent, self.come.at[u], self.place.partner())

    def join(self, u):
        arrive(self.s.at[u], self.come.at[u])

        def one(x):
            for y in range(RING):
                for z in range(RING):
                    t = self.oh[x, y, z] + self.s[u, x, y, z].astype(f32)
                    self.oh[x, y, z] = t
                    self.s[u, x, y, z] = t.astype(bf16)

        loop(RING, one)

    def keep(self, total, u):
        for k, (own,) in total.refs("own"):
            me = self.place.at[ORDERS[k][0]]

            def some(i, k=k, own=own, me=me):
                own[lax.rem(u, total.owns), i] = self.oh[total.piece(k, me, i, ALL) + total.cuts[k]]

            loop(RING, some)

    def finish(self):
        arrive(self.sb, self.sent)


class Down:
    PIECE = (RING, RING, DOWN.rows, DOWN.cols)

    @classmethod
    def scratch(cls):
        return dict(
            hid=pltpu.VMEM((2, T, WIDE), bf16),
            td=pltpu.VMEM((CORES, ROWS_DOWN, D), f32),
            ohd=pltpu.VMEM((2,) + cls.PIECE, f32),
            sbd=pltpu.VMEM((2,) + cls.PIECE, bf16),
            hidsem=sem(2),
            f_snd=sem(2),
        )

    def __init__(self, place, total, refs, hid, come):
        self.place, self.total, self.source, self.come = place, total, hid, come
        self.hid, self.t, self.oh, self.sb, self.sem, self.sent = (refs[n] for n in ("hid", "td", "ohd", "sbd", "hidsem", "f_snd"))

    def block(self, i):
        return self.place.along(X, i + 1)[0]

    def load(self, i):
        slot = lax.rem(i, 2)
        return pltpu.make_async_copy(self.source.at[:, at(self.block(i), WIDE)], self.hid.at[slot], self.sem.at[slot])

    def multiply(self, i, dy):
        slot = lax.rem(i, 2)
        self.load(i).wait()
        when(i + 1 < RING, lambda: self.load(i + 1).start())
        self.t[...] = lax.dot_general(self.hid[slot], dy[...], ROW_BY_ROW, preferred_element_type=f32).reshape(self.t.shape)
        when(i > 1, arrive, self.sb.at[slot], self.sent.at[slot])
        for y in range(RING):
            for z in range(RING):
                row, col = (2 * y + z // 2) * DOWN.rows, (z % 2) * DOWN.cols
                part = (slice(row, row + DOWN.rows), slice(col, col + DOWN.cols))
                self.sb[slot, y, z] = self.t[(1 - self.place.core,) + part].astype(bf16)
                self.oh[slot, y, z] = self.t[(self.place.core,) + part]
        send(self.sb.at[slot], self.total.s.at[0, self.block(i)], self.sent.at[slot], self.come.at[i], self.place.partner())

    def join(self, i):
        slot, x = lax.rem(i, 2), self.block(i)
        s = self.total.s.at[0, x]
        arrive(s, self.come.at[i])

        def one(y):
            for z in range(RING):
                t = self.oh[slot, y, z] + s[y, z].astype(f32)
                self.oh[slot, y, z] = t
                s[y, z] = t.astype(bf16)

        loop(RING, one)
        (_, (p0, first)), (_, (p1, second)), (_, (p2, third)) = self.total.refs("p", "own")
        me, (cut_x, cut_y, cut_z) = self.place.at, self.total.cuts

        def pass_on(k, n, q, to):
            src, dst = ((s.at[(q, ALL) + cut_y], p1.at[0, n, x]), (s.at[(ALL, q) + cut_z], p2.at[0, n, x]))[k - 1]
            send(src, dst, self.total.sem("snd", 0, 0, k), self.total.sem("rcv", 0, 0, k), to)

        for n in OTHERS:
            for k in (1, 2):
                pass_on(k, n - 1, *self.place.along(ORDERS[k][0], n))

        def to_its_chip():
            _, to = self.place.along(X, i + 1)
            send(s.at[(ALL, ALL) + cut_x], p0.at[0, i], self.total.sem("snd", 0, 0, 0), self.total.sem("rcv", 0, 0, 0), to)

        def mine():
            for y in range(RING):
                first[0, y] = self.oh[(slot, y, ALL) + cut_x]

        when(i < RING - 1, to_its_chip)
        when(i == RING - 1, mine)
        for y in range(RING):
            second[0, x, y] = self.oh[(slot, me[Y], y) + cut_y]
            third[0, x, y] = self.oh[(slot, y, me[Z]) + cut_z]

    def run(self, dy, beside=lambda i: None):
        def step(i):
            beside(i)
            within(i, RING, lambda i: self.multiply(i, dy))
            within(i - 1, RING, self.join)

        loop(RING + 1, step)
        for slot in range(2):
            arrive(self.sb.at[slot], self.sent.at[slot])


def normed(h):
    wide = h.astype(f32)
    return (wide * lax.rsqrt(jnp.mean(wide * wide, -1, keepdims=True) + 1e-6)).astype(bf16)


def backward(by, g, u):
    by = by.astype(bf16).astype(f32)
    s = jax.nn.sigmoid(g)
    gated = g * s
    return (by * u * (s * (1.0 + g * (1.0 - s)))).astype(bf16), (by * gated).astype(bf16), (gated * u).astype(bf16)


def call(kernel, name, outs, scratch, collective_id, *args):
    anywhere = pl.BlockSpec(memory_space=pl.ANY)
    return pl.pallas_call(
        functools.partial(kernel, names=tuple(scratch)),
        out_shape=outs,
        in_specs=[anywhere] * len(args),
        out_specs=[anywhere] * len(outs),
        scratch_shapes=list(scratch.values()),
        compiler_params=pltpu.CompilerParams(collective_id=collective_id, has_side_effects=True, vmem_limit_bytes=VMEM_ALL),
        name=name,
    )(*args)


def shape(*dims, dtype=bf16):
    return jax.ShapeDtypeStruct(dims, dtype)


def named(names, scratch):
    return dict(zip(names, scratch, strict=True))


GATHERED = (CHUNKS, 2, RING, CORES, ROWS, N)


def first_kernel(x, w_gate, w_up, w_down, a_out, hid_out, gu_out, d_out, *scratch, names):
    refs = named(names, scratch)
    a, hs, gs, xsem, asem, hsem, gsem = (refs[n] for n in ("a", "hs", "gs", "xsem", "asem", "hsem", "gsem"))
    load = pltpu.make_async_copy(x, a, xsem)
    load.start()
    place = Place()
    place.meet()
    gather = Gather(place, refs, refs["w"], (w_gate, w_up), 0)
    down = DownGather(place, refs, d_out, w_down, 0)
    for j in range(3):
        gather.start_x(j)
    down.load.start()
    load.wait()

    def norm(i):
        a[at(i, 64)] = normed(a[at(i, 64)])

    loop(T // 64, norm)
    keep = pltpu.make_async_copy(a, a_out, asem)
    keep.start()

    def outs(j, i):
        return (
            pltpu.make_async_copy(hs.at[i], hid_out.at[at(i, TILE), at(j, N)], hsem.at[i]),
            pltpu.make_async_copy(gs.at[i], gu_out.at[j, :, at(i, TILE)], gsem.at[i]),
        )

    def compute(j):
        gather.ready(j)

        def tile(i):
            when(j > 0, lambda: wait(outs(j, i)))
            g, u = (jnp.dot(a[at(i, TILE)], gather.w[j, m].reshape(D, N), preferred_element_type=f32) for m in range(2))
            gs[i, 0], gs[i, 1] = g, u
            hs[i] = (g * jax.nn.sigmoid(g) * u).astype(bf16)
            start(outs(j, i))

        loop(T // TILE, tile)

    def step(t):
        within(t, CHUNKS, gather.start_yz)
        within(t + 3, CHUNKS, gather.start_x)
        within(t - 1, CHUNKS, gather.start_d)
        for stage, lag in ((down.start_x, 4), (down.start_yz, 6), (down.start_d, 7)):
            within(t - lag, down.UNITS, stage)
        within(t - 2, CHUNKS, compute)

    loop(CHUNKS + down.UNITS, step)
    down.finish()
    gather.finish()
    keep.wait()
    for i in range(T // TILE):
        wait(outs(CHUNKS - 1, i))


def first(x, w_gate, w_up, w_down, collective_id):
    scratch = dict(
        Gather.scratch(),
        **DownGather.scratch(),
        w=pltpu.VMEM(GATHERED, bf16),
        a=pltpu.VMEM((T, D), bf16),
        hs=pltpu.VMEM((T // TILE, TILE, N), bf16),
        gs=pltpu.VMEM((T // TILE, 2, TILE, N), f32),
        xsem=sem(),
        asem=sem(),
        hsem=sem(2),
        gsem=sem(2),
    )
    outs = (shape(T, D), shape(T, F), shape(CHUNKS, 2, T, N, dtype=f32), shape(RING, CORES, ROWS_DOWN, D))
    return call(first_kernel, "first", outs, scratch, collective_id, x, w_gate, w_up, w_down)


SHORT = 512


def second_kernel(x, hid, d, w_down, h_out, a_out, d1_out, *scratch, names):
    refs = named(names, scratch)
    dv, hv, xv, ho, ao, dsem, hsem, xsem, osem = (refs[n] for n in ("dv", "hv", "xv", "ho", "ao", "dsem", "hsem", "xsem", "osem"))

    def loads(i, slot):
        return (
            pltpu.make_async_copy(hid.at[at(i, SHORT)], hv.at[slot], hsem.at[slot]),
            pltpu.make_async_copy(x.at[at(i, SHORT)], xv.at[slot], xsem.at[slot]),
        )

    def stores(i, slot):
        pairs = ((ho, h_out), (ao, a_out))
        return [pltpu.make_async_copy(v.at[slot], out.at[at(i, SHORT)], osem.at[n, slot]) for n, (v, out) in enumerate(pairs)]

    load = pltpu.make_async_copy(d, dv, dsem)
    load.start()
    start(loads(0, 0))
    place = Place()
    place.meet()
    down = DownGather(place, refs, d1_out, w_down, 1)
    down.load.start()
    loop(down.UNITS, down.start_x)
    load.wait()

    def compute(i):
        slot = lax.rem(i, 2)
        wait(loads(i, slot))
        when(i + 1 < T // SHORT, lambda: start(loads(i + 1, 1 - slot)))
        when(i > 1, lambda: wait(stores(i, slot)))
        h = xv[slot] + jnp.dot(hv[slot], dv[...].reshape(F, D), preferred_element_type=f32).astype(bf16)
        ho[slot] = h
        ao[slot] = normed(h)
        start(stores(i, slot))

    def step(t):
        within(t, T // SHORT, compute)
        within(t, down.UNITS, down.start_yz)
        within(t - 1, down.UNITS, down.start_d)

    loop(down.UNITS + 1, step)
    down.finish()
    for slot in range(2):
        wait(stores(0, slot))


def second(x, hid, d, w_down, collective_id):
    pair = pltpu.VMEM((2, SHORT, D), bf16)
    scratch = dict(
        DownGather.scratch(),
        dv=pltpu.VMEM((RING, CORES, ROWS_DOWN, D), bf16),
        hv=pltpu.VMEM((2, SHORT, F), bf16),
        xv=pair,
        ho=pair,
        ao=pair,
        dsem=sem(),
        hsem=sem(2),
        xsem=sem(2),
        osem=sem(2, 2),
    )
    outs = (shape(T, D), shape(T, D), shape(RING, CORES, ROWS_DOWN, D))
    return call(second_kernel, "second", outs, scratch, collective_id, x, hid, d, w_down)


EARLY = gate_up_sum("e_", 3)
LATE = gate_up_sum("l_", CHUNKS - EARLY.units, CHUNKS - EARLY.units)


def third_kernel(a_in, dy_in, d, w_gate, w_up, hid_out, dg_out, du_out, w_out, ga_out, s_out, oh_out, *scratch, names):
    refs = named(names, scratch)
    a, dy, dv, wv, side, lsem, dsem, vsem, osem, ksem = (refs[n] for n in ("a", "dy", "dv", "wv", "side", "lsem", "dsem", "vsem", "osem", "ksem"))
    blocks = refs["blocks"]
    pairs = ((w_gate.at[1], blocks.at[0]), (w_up.at[1], blocks.at[1]), (a_in, a), (dy_in, dy))
    loads = [pltpu.make_async_copy(*pair, lsem.at[n]) for n, pair in enumerate(pairs)]
    start(loads)

    def operands(j):
        slot = lax.rem(j, 2)
        return (
            pltpu.make_async_copy(d.at[at(j, N)], dv.at[slot], dsem.at[slot]),
            pltpu.make_async_copy(w_out.at[j], wv.at[slot], vsem.at[slot]),
        )

    place = Place()
    place.meet()
    gather = Gather(place, refs, w_out, (w_gate, w_up), 1, blocks)
    wait(loads[:2])
    s = refs["s"]
    total = EARLY.bind(place, refs, s)
    grads = GateUp(place, refs, s, refs["come"])
    for j in range(3):
        gather.start_x(j)
    wait(loads[2:])

    def fetch(j):
        gather.ready(j)
        start(operands(j))

    def outs(j):
        return [pltpu.make_async_copy(side.at[n], out.at[:, at(j, N)], osem.at[n]) for n, out in enumerate((dg_out, du_out, hid_out))]

    def leave(u):
        late = u - EARLY.units
        return (pltpu.make_async_copy(s.at[u], s_out.at[late], ksem.at[0]), pltpu.make_async_copy(grads.oh, oh_out.at[late], ksem.at[1]))

    def join(u):
        grads.join(u)

        def go_on():
            grads.keep(total, u)
            total.start1(u)

        when(u < EARLY.units, go_on)
        when(u >= EARLY.units, lambda: start(leave(u)))

    def compute(j):
        slot = lax.rem(j, 2)
        wait(operands(j))
        when(j > 0, lambda: wait(outs(j)))

        def tile(i):
            rows = at(i, TILE)
            g, u = (jnp.dot(a[rows], wv[slot, m].reshape(D, N), preferred_element_type=f32) for m in range(2))
            by = lax.dot_general(dy[rows], dv[slot], BY_LAST, preferred_element_type=f32)
            side[0, rows], side[1, rows], side[2, rows] = backward(by, g, u)

        loop(T // TILE, tile)
        start(outs(j))
        within(j + 1, CHUNKS, fetch)
        total.stages(j - 1)
        within(j - 1, CHUNKS, join)
        grads.multiply(j, a, (side.at[0], side.at[1]), lambda: when(j > EARLY.units, lambda: wait(leave(j - 1))))

    def step(t):
        within(t, CHUNKS, gather.start_yz)
        within(t + 3, CHUNKS, gather.start_x)
        within(t - 1, CHUNKS, gather.start_d)
        when(t == 1, fetch, 0)
        within(t - 2, CHUNKS, compute)

    loop(CHUNKS + 2, step)
    total.stages(CHUNKS - 1)
    join(CHUNKS - 1)
    total.stages(CHUNKS)
    wait(leave(CHUNKS - 1))
    grads.finish()
    gather.finish()
    total.finish()
    wait(outs(CHUNKS - 1))
    keep = pltpu.make_async_copy(total.ga, ga_out, ksem.at[0])
    keep.start()
    keep.wait()


def third(a, dy, d, w_gate, w_up, collective_id):
    pieces = (RING, RING, RING, ROWS // 2, LANES)
    early = EARLY.scratch()
    del early["e_s"]
    scratch = dict(
        Gather.scratch(),
        **GateUp.scratch(),
        **early,
        s=pltpu.VMEM((CHUNKS,) + pieces, bf16),
        come=sem(CHUNKS),
        a=pltpu.VMEM((T, D), bf16),
        dy=pltpu.VMEM((T, D), bf16),
        dv=pltpu.VMEM((2, N, D), bf16),
        wv=pltpu.VMEM((2,) + GATHERED[1:], bf16),
        side=pltpu.VMEM((3, T, N), bf16),
        blocks=pltpu.VMEM((2, ROWS, F), bf16),
        lsem=sem(4),
        dsem=sem(2),
        vsem=sem(2),
        osem=sem(3),
        ksem=sem(2),
    )
    outs = [shape(T, F)] * 3 + [shape(*GATHERED), shape(EARLY.units, RING, RING, ROWS // 2, LANES)]
    outs += [shape(LATE.units, *pieces), shape(LATE.units, *pieces, dtype=f32)]
    return call(third_kernel, "third", outs, scratch, collective_id, a, dy, d.reshape(F, D), w_gate, w_up)


def fourth_kernel(hid, dy_in, dg, du, w, h, s_in, oh_in, dh_out, ga_out, gd_out, *scratch, names):
    refs = named(names, scratch)
    dy, lsem, csem, osem = (refs[n] for n in ("dy", "lsem", "csem", "osem"))
    load = pltpu.make_async_copy(dy_in, dy, lsem)
    load.start()
    place = Place()
    late, low = LATE.bind(place, refs), DOWN.bind(place, refs)
    carried = [pltpu.make_async_copy(s_in, late.s, csem.at[3])]
    for k, (own,) in late.refs("own"):
        pieces = (ALL,) + late.piece(k, place.at[ORDERS[k][0]]) + late.cuts[k]
        carried.append(pltpu.make_async_copy(oh_in.at[pieces], own, csem.at[k]))
    start(carried)
    place.meet()
    wait(carried)

    def late_stages(t):
        late.stages(t)
        within(t, late.units, late.start1)

    late_stages(0)

    def multiply_down(**refs_down):
        down = Down(place, low, refs_down, hid, refs["come"])
        down.load(0).start()
        load.wait()
        down.run(dy)

    pl.run_scoped(multiply_down, **Down.scratch())

    def multiply_back(gv, wv, acc, hv, gsem, hsem):
        def loads(j, slot):
            yield pltpu.make_async_copy(w.at[j], wv.at[slot], gsem.at[slot, 2])
            for n, side in enumerate((dg, du)):
                yield pltpu.make_async_copy(side.at[:, at(j, N)], gv.at[slot, n], gsem.at[slot, n])

        start(loads(0, 0))

        def step(j):
            slot = lax.rem(j, 2)
            wait(loads(j, slot))
            when(j + 1 < CHUNKS, lambda: start(loads(j + 1, 1 - slot)))
            late_stages(j + 1)
            low.stages(j)

            def tile(i):
                rows = at(i, SHORT)
                by, more = (lax.dot_general(gv[slot, m, rows], wv[slot, m].reshape(D, N), BY_LAST, preferred_element_type=f32) for m in range(2))
                by += more

                def first_time():
                    acc[rows] = by

                def again():
                    acc[rows] += by

                when(j == 0, first_time)
                when(j > 0, again)

            loop(T // SHORT, tile)

        loop(CHUNKS, step)

        def tile_of_h(i):
            slot = lax.rem(i, 2)
            return pltpu.make_async_copy(h.at[at(i, 256)], hv.at[slot], hsem.at[slot])

        tile_of_h(0).start()
        late_stages(CHUNKS + 1)

        def norm(i):
            tile_of_h(i).wait()
            when(i + 1 < T // 256, lambda: tile_of_h(i + 1).start())

            def part(n):
                rows = pl.ds(pl.multiple_of(i * 256 + n * 64, 64), 64)
                wide = hv[lax.rem(i, 2), at(n, 64)].astype(f32)
                by = acc[rows].astype(bf16).astype(f32)
                scale = lax.rsqrt(jnp.mean(wide * wide, -1, keepdims=True) + 1e-6)
                along = jnp.mean(by * wide, -1, keepdims=True)
                dy[rows] = dy[rows] + (by * scale - wide * (scale * scale * scale * along)).astype(bf16)

            loop(4, part)

        loop(T // 256, norm)

    pl.run_scoped(
        multiply_back,
        pltpu.VMEM((2, 2, T, N), bf16),
        pltpu.VMEM((2,) + GATHERED[1:], bf16),
        pltpu.VMEM((T, D), f32),
        pltpu.VMEM((2, 256, D), bf16),
        sem(2, 3),
        sem(2),
    )
    results = [pltpu.make_async_copy(v, out, osem.at[n]) for n, (v, out) in enumerate(((dy, dh_out), (late.ga, ga_out), (low.ga.at[0], gd_out)))]
    start(results)
    late.finish()
    low.finish()
    wait(results)


def fourth(hid, dy, dg, du, w, h, s, oh, collective_id):
    scratch = dict(
        LATE.scratch(),
        **DOWN.scratch(),
        come=sem(RING),
        dy=pltpu.VMEM((T, D), bf16),
        lsem=sem(),
        csem=sem(4),
        osem=sem(3),
    )
    outs = [shape(T, D), shape(LATE.units, RING, RING, ROWS // 2, LANES), shape(*Down.PIECE)]
    return call(fourth_kernel, "fourth", outs, scratch, collective_id, hid, dy, dg, du, w, h, s, oh)


LAST = gate_up_sum("e_", CHUNKS)


def fifth_kernel(hid, dy_in, a_in, d, gu, ga_early, ga_late, gd_in, ga_out, gd_out, sum_out, *scratch, names):
    refs = named(names, scratch)
    dy, lsem, osem = (refs[n] for n in ("dy", "lsem", "osem"))
    load = pltpu.make_async_copy(dy_in, dy, lsem)
    load.start()
    place = Place()
    others = place.shard_group()
    place.meet(others)
    total, low = LAST.bind(place, refs), DOWN.bind(place, refs)

    def multiply_down(**refs_down):
        down = Down(place, low, refs_down, hid, refs["come"])
        down.load(0).start()
        load.wait()
        down.run(dy)

    pl.run_scoped(multiply_down, **Down.scratch())
    tiles, ahead = T // SHORT, 3

    def multiply_gates(a, dv, gv, side, asem, dsem, gsem, **refs_grads):
        grads = GateUp(place, refs_grads, total.s, refs["arrived"])
        load_a = pltpu.make_async_copy(a_in, a, asem)

        def rows_of_d(j):
            return pltpu.make_async_copy(d.at[at(j, N)], dv, dsem)

        def tile_of_gu(n):
            slot = lax.rem(n, ahead)
            return pltpu.make_async_copy(gu.at[n // tiles, :, at(lax.rem(n, tiles), SHORT)], gv.at[slot], gsem.at[slot])

        start([rows_of_d(0), load_a] + [tile_of_gu(n) for n in range(ahead)])

        def join(u):
            grads.join(u)
            grads.keep(total, u)
            total.start1(u)

        def back(j):
            rows_of_d(j).wait()

            def tile(i):
                n = j * tiles + i
                tile_of_gu(n).wait()
                by = lax.dot_general(dy[at(i, SHORT)], dv[...], BY_LAST, preferred_element_type=f32)
                side[0, at(i, SHORT)], side[1, at(i, SHORT)], _ = backward(by, gv[lax.rem(n, ahead), 0], gv[lax.rem(n, ahead), 1])
                when(n + ahead < CHUNKS * tiles, lambda: tile_of_gu(n + ahead).start())

            loop(tiles, tile)
            when(j + 1 < CHUNKS, lambda: rows_of_d(j + 1).start())

        def step(t):
            within(t, CHUNKS, back)
            low.stages(t)
            total.stages(t - 1)
            within(t - 1, CHUNKS, join)
            when(t == 0, load_a.wait)
            within(t, CHUNKS, lambda j: grads.multiply(j, a, (side.at[0], side.at[1])))

        loop(CHUNKS + 1, step)
        grads.finish()

    pl.run_scoped(
        multiply_gates,
        pltpu.VMEM((T, D), bf16),
        pltpu.VMEM((N, D), bf16),
        pltpu.VMEM((ahead, 2, SHORT, N), f32),
        pltpu.VMEM((2, T, N), bf16),
        sem(),
        sem(),
        sem(ahead),
        **GateUp.scratch(),
    )

    def square(g, d, gsem):
        loads = [pltpu.make_async_copy(*pair, gsem.at[n]) for n, pair in enumerate(((ga_early, g.at[:EARLY.units]), (ga_late, g.at[EARLY.units :]), (gd_in, d)))]
        start(loads)
        total.stages(CHUNKS)
        squares = refs["squares"]
        me = place.at[X] * CORES + place.core
        mine = squares.at[me]
        mine[...] = jnp.zeros(mine.shape, f32)

        def add(piece):
            for n in range(0, piece.shape[1], LANES):
                t = piece[:, n : n + LANES].astype(f32)
                mine[...] += jnp.sum((t * t).reshape((-1,) + mine.shape), 0)

        def add_all(all_gates, all_down):
            loop(CHUNKS * RING, lambda i: [add(all_gates[i // RING, lax.rem(i, RING), z]) for z in range(RING)])
            loop(RING, lambda y: [add(all_down[y, z]) for z in range(RING)])

        wait(loads)
        add_all(g, d)
        loop(4, lambda t: total.stages(t + CHUNKS + 1))
        add_all(total.ga, low.ga.at[0])
        for to in others + [place.partner()] + [place.along(X, k)[1] for k in OTHERS]:
            send(mine, mine, refs["q_snd"], refs["q_rcv"], to)
        for semaphore in (refs["q_rcv"], refs["q_snd"]):
            arrive(squares.at[: BLOCKS - 1], semaphore)
        sum_ref = refs["sum"]
        sum_ref[...] = squares[0]
        for n in range(1, BLOCKS):
            sum_ref[...] += squares[n]

    pl.run_scoped(square, pltpu.VMEM(total.ga.shape, bf16), pltpu.VMEM(Down.PIECE, bf16), sem(3))
    results = [pltpu.make_async_copy(v, out, osem.at[n]) for n, (v, out) in enumerate(((total.ga, ga_out), (low.ga.at[0], gd_out), (refs["sum"], sum_out)))]
    start(results)
    total.finish()
    low.finish()
    wait(results)


def fifth(hid, dy, a, d, gu, *layer1, collective_id):
    scratch = dict(
        LAST.scratch(),
        **DOWN.scratch(),
        come=sem(RING),
        arrived=sem(CHUNKS),
        dy=pltpu.VMEM((T, D), bf16),
        lsem=sem(),
        osem=sem(3),
        squares=pltpu.VMEM((BLOCKS, 8, LANES), f32),
        sum=pltpu.VMEM((8, LANES), f32),
        q_snd=sem(),
        q_rcv=sem(),
    )
    outs = [shape(CHUNKS, RING, RING, ROWS // 2, LANES), shape(*Down.PIECE), shape(8, LANES, dtype=f32)]
    return call(fifth_kernel, "fifth", outs, scratch, collective_id, hid, dy, a, d.reshape(F, D), gu, *layer1)


SLOTS = 4
TALL = 2 * 2 * DOWN.rows


def sixth_kernel(*args, names):
    (total, *gradients), args = args[:6], args[6:]
    weights, outs, refs = args[:9], args[9:18], named(names, args[18:])
    g1, g0, d1, d0, sv = (refs[n] for n in ("g1", "g0", "d1", "d0", "sv"))
    early, late, down1, both0, down0 = gradients
    pairs = ((total, sv), (early, g1.at[: EARLY.units]), (late, g1.at[EARLY.units :]), (both0, g0), (down1, d1), (down0, d0))
    loads = [pltpu.make_async_copy(*pair, refs["lsem"].at[n]) for n, pair in enumerate(pairs)]
    start(loads)

    def copies(n, arrays, into, which, kind):
        per, rows, buffers = (RING, ROWS // 2, ("gw", "gm", "gv")) if kind < 2 else (2, TALL, ("dw", "dm", "dv"))
        slot = lax.rem(n, SLOTS)
        for i, buffer in enumerate(buffers):
            there, here = arrays[3 * i + kind].at[n // per, at(lax.rem(n, 2), rows)], refs[buffer].at[slot]
            yield pltpu.make_async_copy(*((there, here) if into else (here, there)), refs["sems"].at[which, kind // 2, slot, i])

    def gates(n, do, arrays, into, which):
        for kind in range(2):
            when(lax.rem(n, RING) // 2 == kind, lambda kind=kind: do(copies(n, arrays, into, which, kind)))

    def downs(n, do, arrays, into, which):
        do(copies(n, arrays, into, which, 2))

    wait(loads[:1])
    squares = jnp.sum(sv[...], keepdims=True)
    factor = jnp.minimum(1.0, 0.5 * lax.rsqrt(squares / (LAYERS * 3 * D * F) + 1e-30))

    def adamw(slot, buffers, part, g):
        w, m, v = (refs[b].at[slot] for b in buffers)
        g = g.astype(f32) * factor
        new_m = 0.9 * m[part] + 0.1 * g
        new_v = 0.95 * v[part] + 0.05 * g * g
        old = w[part].astype(f32)
        w[part] = (old - 0.02 * (new_m * lax.rsqrt(new_v + 1e-8) + 0.1 * old)).astype(bf16)
        m[part], v[part] = new_m, new_v

    def run(steps, transfer, body):
        for n in range(SLOTS - 1):
            transfer(jnp.int32(n), start, weights, True, 0)

        def step(n):
            transfer(n, wait, weights, True, 0)
            body(n, lax.rem(n, SLOTS))
            transfer(n, start, outs, False, 1)
            when(n > 0, lambda: transfer(n - 1, wait, outs, False, 1))
            within(n + SLOTS - 1, steps, lambda n: transfer(n, start, weights, True, 0))

        loop(steps, step)
        transfer(jnp.int32(steps - 1), wait, outs, False, 1)

    def gate_step(n, slot):
        def of(g):
            for j in range(CHUNKS):
                for y in range(RING):
                    columns = slice(j * N + y * LANES, j * N + (y + 1) * LANES)
                    adamw(slot, ("gw", "gm", "gv"), (ALL, columns), g[j, y, lax.rem(n, RING)])

        when(n < RING, of, g0)
        when(n >= RING, of, g1)

    def down_step(n, slot):
        def of(d):
            for y in range(2):
                for z in range(RING):
                    row, col = (2 * y + z // 2) * DOWN.rows, (z % 2) * DOWN.cols
                    part = (slice(row, row + DOWN.rows), slice(col, col + DOWN.cols))
                    adamw(slot, ("dw", "dm", "dv"), part, d[2 * lax.rem(n, 2) + y, z])

        when(n < 2, of, d0)
        when(n >= 2, of, d1)

    wait(loads[1:])
    run(LAYERS * RING, gates, gate_step)
    run(LAYERS * 2, downs, down_step)


def sixth(total, gradients, weights):
    half, tall = (SLOTS, ROWS // 2, F), (SLOTS, TALL, D)
    pieces = pltpu.VMEM((CHUNKS, RING, RING, ROWS // 2, LANES), bf16)
    scratch = dict(g1=pieces, g0=pieces, d1=pltpu.VMEM(Down.PIECE, bf16), d0=pltpu.VMEM(Down.PIECE, bf16), sv=pltpu.VMEM((8, LANES), f32))
    for name, dims in (("g", half), ("d", tall)):
        scratch.update({name + "w": pltpu.VMEM(dims, bf16), name + "m": pltpu.VMEM(dims, f32), name + "v": pltpu.VMEM(dims, f32)})
    scratch.update(lsem=sem(6), sems=sem(2, 2, SLOTS, 3))
    outs = [shape(*w.shape, dtype=w.dtype) for w in weights]
    return call(sixth_kernel, "sixth", outs, scratch, None, total, *gradients, *weights)


def solution(mesh):
    def step(x, dy, *arrays):
        w_gate, w_up, w_down = arrays[:3]
        x, dy = x[0], dy[0]
        a0, hid0, gu0, d0 = first(x, w_gate, w_up, w_down, 0)
        h1, a1, d1 = second(x, hid0, d0, w_down, 1)
        hid1, dg1, du1, w1, early, s, oh = third(a1, dy, d1, w_gate, w_up, 2)
        dh1, late, down1 = fourth(hid1, dy, dg1, du1, w1, h1, s, oh, 3)
        both0, down0, total = fifth(hid0, dh1, a0, d0, gu0, early, late, down1, collective_id=4)
        return tuple(sixth(total, (early, late, down1, both0, down0), arrays))

    states, cut = P(("rep", "r", "s"), None, None), P(None, "s", None)
    return jax.shard_map(
        step,
        mesh=mesh,
        in_specs=(states, states) + (cut,) * 9,
        out_specs=(P("rep", "s", None),) * 9,
        check_vma=False,
    )
```

```python
import functools

import jax
import jax.numpy as jnp
from jax import lax
from jax.experimental import pallas as pl
from jax.experimental.pallas import tpu as pltpu
from jax.sharding import PartitionSpec as P

bf16, f32 = jnp.bfloat16, jnp.float32
MESH = pl.DeviceIdType.MESH
VMEM_ALL = 67043328
T, D, F, LAYERS = 2048, 1280, 3584, 2
CORES, RING, LANES = 2, 4, 128
BLOCKS = RING * CORES
N, TILE = 512, 1024
CHUNKS = F // N
ROWS, ROWS_DOWN = D // BLOCKS, F // BLOCKS
WIDE = F // RING
X, Y, Z = range(3)
AXES = (X, Y, Z)
ORDERS = ((X, Y, Z), (Y, Z, X), (Z, X, Y))
OTHERS = (1, 3, 2)
ALL = slice(None)
ROW_BY_ROW, BY_LAST = (((0,), (0,)), ((), ())), (((1,), (1,)), ((), ()))


def at(i, n):
    return pl.ds(pl.multiple_of(i * n, n), n)


def sem(*shape):
    return pltpu.SemaphoreType.DMA(shape)


def loop(n, body):
    def step(i, none):
        body(i)
        return none

    lax.fori_loop(0, n, step, 0)


def when(condition, do, *args):
    pl.when(condition)(functools.partial(do, *args))


def within(t, n, stage):
    when((t >= 0) & (t < n), stage, t)


def start(copies):
    for copy in copies:
        copy.start()


def wait(copies):
    for copy in copies:
        copy.wait()


def arrive(ref, semaphore):
    pltpu.make_async_copy(ref, ref, semaphore).wait()


def send(src, dst, sent, come, to):
    pltpu.make_async_remote_copy(src_ref=src, dst_ref=dst, send_sem=sent, recv_sem=come, device_id=to, device_id_type=MESH).start()


class Place:
    def __init__(self):
        r, s = lax.axis_index("r"), lax.axis_index("s")
        self.rep = lax.axis_index("rep")
        self.core = lax.rem(s, CORES)
        self.at = (s // CORES, r // RING, lax.rem(r, RING))

    def id(self, x, y, z, core):
        return (self.rep, y * RING + z, x * CORES + core)

    def along(self, axis, k):
        there = list(self.at)
        there[axis] = lax.rem(there[axis] + k, RING)
        return there[axis], self.id(*there, self.core)

    def partner(self):
        return self.id(*self.at, 1 - self.core)

    def shard_group(self):
        x, y, z = self.at
        return [self.id(lax.rem(x + k, RING), y, z, 1 - self.core) for k in OTHERS]

    def meet(self, more=()):
        barrier = pltpu.get_barrier_semaphore()
        ids = [self.partner()] + [self.along(a, k)[1] for a in AXES for k in OTHERS] + list(more)
        for i in ids:
            pl.semaphore_signal(barrier, device_id=i, device_id_type=MESH)
        pl.semaphore_wait(barrier, len(ids))


BOTH = ((1, 0), (3, 1))


class Fetch:
    REST, STAGES = slice(1, RING), range(4)

    def __init__(self, place, refs, w, source):
        self.place, self.w, self.source = place, w, source
        self.own, self.snd, self.rcv = (refs[self.name + n] for n in ("own", "snd", "rcv"))
        _, y, z = place.at
        self.parts = [pl.ds(pl.multiple_of(self.alone + self.quarter * i, 16), self.quarter) for i in (y, RING + z)]

    @classmethod
    def scratch(cls):
        shape = (len(cls.STAGES), cls.units)
        return {cls.name + "own": sem(cls.units), cls.name + "snd": sem(*shape), cls.name + "rcv": sem(*shape)}

    def copy(self, stage, u, to, src, dst=None):
        send(src, src if dst is None else dst, self.snd.at[stage, u], self.rcv.at[stage, u], to)

    def came(self, stage, u, semaphores):
        rows = self.alone + 2 * self.quarter
        blocks, rows = ((2, rows), (1, rows), (3, 2 * 3 * self.quarter), (RING, self.all_rows))[stage]
        arrive(self.block(u, pl.ds(0, blocks), pl.ds(0, rows)), semaphores.at[stage, u])

    def along_x(self):
        return [(k, half, rows, self.place.along(X, k)[1]) for k, half in BOTH for rows in [pl.ds(0, self.alone)] + self.parts]

    def start_x(self, u):
        for k, _, rows, to in self.along_x():
            self.copy(0, u, to, self.mine(u, rows), self.block(u, RING - k, rows))
        pltpu.make_async_copy(self.mine(u, ALL), self.block(u, 0, ALL), self.own.at[u]).start()

    def pass_x(self, u):
        self.came(0, u, self.rcv)
        for k, half, rows, to in self.along_x():
            self.copy(1, u, to, self.block(u, RING - k, rows, half), self.block(u, 2, rows, half))

    def start_yz(self, u):
        self.came(1, u, self.rcv)
        for k in OTHERS:
            for axis, rows in zip((Y, Z), self.parts, strict=True):
                self.copy(2, u, self.place.along(axis, k)[1], self.block(u, self.REST, rows))

    def start_d(self, u):
        self.came(2, u, self.rcv)
        arrive(self.block(u, 0, ALL), self.own.at[u])
        self.copy(3, u, self.place.partner(), self.block(u, ALL, ALL))

    def ready(self, u):
        self.came(3, u, self.rcv)

    def finish(self):
        def one(u):
            for stage in self.STAGES:
                self.came(stage, u, self.snd)

        loop(self.units, one)


class Gather(Fetch):
    name, units, alone, quarter, all_rows = "g_", LAYERS * CHUNKS, 32, 16, ROWS

    def block(self, u, chips, rows, half=ALL):
        return self.w.at[u // CHUNKS, lax.rem(u, CHUNKS), half, chips, self.place.core, rows]

    def mine(self, u, rows):
        return self.source.at[u // CHUNKS, :, rows, at(lax.rem(u, CHUNKS), N)]


class DownGather(Fetch):
    parted = 5
    name, units, alone, quarter, all_rows = "d_", LAYERS * parted, 64, 48, ROWS_DOWN

    def columns(self, u, half=None):
        u, n = lax.rem(u, self.parted), D // self.parted
        return at(u, n) if half is None else at(2 * u + half, n // 2)

    def block(self, u, chips, rows, half=None):
        return self.w.at[u // self.parted, chips, self.place.core, rows, self.columns(u, half)]

    def mine(self, u, rows):
        return self.source.at[u // self.parted, rows, self.columns(u)]


def chunk_of(place, w, j, into, semaphore):
    return [pltpu.make_async_copy(w.at[j, :, k], into.at[:, place.along(X, k)[0]], semaphore) for k in range(RING)]


def hidden_rows(place, d, j, into, semaphore):
    for i in range(N // LANES):
        n = j * (N // LANES) + i
        k = lax.rem(n // CHUNKS + RING - place.at[X], RING)
        yield pltpu.make_async_copy(d.at[k, at(lax.rem(n, CHUNKS), LANES)], into.at[at(i, LANES)], semaphore)


class Sum:
    def __init__(self, name, units, rows, cols, cuts, owns=1):
        self.name, self.units, self.rows, self.cols, self.cuts, self.owns = name, units, rows, cols, cuts, owns

    def scratch(self):
        u, piece = self.units, (self.rows, self.cols)
        shapes = dict(s=pltpu.VMEM((u, RING, RING, RING) + piece, bf16), ga=pltpu.VMEM((u, RING, RING) + piece, bf16))
        for k, (r, c) in enumerate(self.cuts):
            part = (r.stop - r.start, c.stop - c.start)
            shapes[f"own{k}"] = pltpu.VMEM((self.owns, RING, RING) + part, f32)
            if self.owns < u:
                shapes[f"one{k}"] = pltpu.VMEM((RING, RING) + part, f32)
            shapes[f"two{k}"] = pltpu.VMEM((RING,) + part, f32)
            shapes[f"p{k}"] = pltpu.VMEM((u, 3, RING, RING) + part, bf16)
            shapes[f"q{k}"] = pltpu.VMEM((u, 3, RING) + part, bf16)
            shapes[f"r{k}"] = pltpu.VMEM((u, 3) + part, bf16)
        shapes.update(snd=sem(5, u, 3), rcv=sem(5, u, 3))
        return {self.name + key: value for key, value in shapes.items()}

    def bind(self, place, refs, s=None):
        self.place = place
        self.ref = {key[len(self.name) :]: ref for key, ref in refs.items() if key.startswith(self.name)}
        self.s, self.ga = self.ref["s"] if s is None else s, self.ref["ga"]
        return self

    def refs(self, *names):
        return [(k, [self.ref[f"{name}{k}"] for name in names]) for k in AXES]

    def ones(self, k, u):
        return self.ref[f"one{k}"] if self.owns < self.units else self.ref[f"own{k}"].at[u]

    def piece(self, k, q, *rest):
        rest = list(rest) or [ALL, ALL]
        return tuple(q if a == ORDERS[k][0] else rest.pop(0) for a in AXES)

    def sem(self, name, stage, u, k):
        return self.ref[name].at[stage, u, k]

    def pass_on(self, stage, u, k, axis, pair):
        for n in OTHERS:
            q, to = self.place.along(axis, n)
            send(*pair(q, n - 1), self.sem("snd", stage, u, k), self.sem("rcv", stage, u, k), to)

    def start1(self, u):
        for k, (p,) in self.refs("p"):
            self.pass_on(0, u, k, ORDERS[k][0], lambda q, n, k=k, p=p: (self.s.at[(u,) + self.piece(k, q) + self.cuts[k]], p.at[u, n]))

    def leading(self, k):
        return ORDERS[k][1] < ORDERS[k][2]

    def add1(self, u):
        for k, (p, q, own) in self.refs("p", "q", "own"):
            one = self.ones(k, u)
            arrive(p.at[u], self.sem("rcv", 0, u, k))

            def some(i, p=p, own=own, one=one):
                t = own[lax.rem(u, self.owns), i] + p[u, 0, i].astype(f32) + p[u, 1, i].astype(f32) + p[u, 2, i].astype(f32)
                one[i] = t
                p[u, 0, i] = t.astype(bf16)

            loop(RING, some)
            self.pass_on(1, u, k, ORDERS[k][1], lambda i, n, k=k, p=p, q=q: (p.at[(u, 0, i) if self.leading(k) else (u, 0, ALL, i)], q.at[u, n]))

    def add2(self, u):
        for k, (q, r, two) in self.refs("q", "r", "two"):
            one = self.ones(k, u)
            arrive(q.at[u], self.sem("rcv", 1, u, k))
            me = self.place.at[ORDERS[k][1]]
            for i in range(RING):
                mine = one[me, i] if self.leading(k) else one[i, me]
                t = mine + q[u, 0, i].astype(f32) + q[u, 1, i].astype(f32) + q[u, 2, i].astype(f32)
                two[i] = t
                q[u, 0, i] = t.astype(bf16)
            self.pass_on(2, u, k, ORDERS[k][2], lambda i, n, q=q, r=r: (q.at[u, 0, i], r.at[u, n]))

    def line(self, u, z):
        return self.ga.at[u, self.place.at[Y], z]

    def add3(self, u):
        _, y, z = self.place.at
        for k, (r, two) in self.refs("r", "two"):
            arrive(r.at[u], self.sem("rcv", 2, u, k))
            t = two[self.place.at[ORDERS[k][2]]] + r[u, 0].astype(f32) + r[u, 1].astype(f32) + r[u, 2].astype(f32)
            self.ga[(u, y, z) + self.cuts[k]] = t.astype(bf16)
        self.pass_on(3, u, 0, Z, lambda q, n: [self.line(u, z)] * 2)

    def three(self, u, name, stage):
        arrive(self.ga.at[u, pl.ds(0, 3), 0 if stage == 3 else ALL], self.sem(name, stage, u, 0))

    def gather(self, u):
        self.three(u, "rcv", 3)
        self.pass_on(4, u, 0, Y, lambda q, n: [self.line(u, ALL)] * 2)

    def gathered(self, u):
        self.three(u, "rcv", 4)

    def finish(self):
        def one(u):
            for k, parts in self.refs("p", "q", "r"):
                for stage, part in enumerate(parts):
                    arrive(part.at[u], self.sem("snd", stage, u, k))
            for stage in (3, 4):
                self.three(u, "snd", stage)

        loop(self.units, one)

    def stages(self, t):
        for lag, stage in enumerate((self.gathered, self.gather, self.add3, self.add2, self.add1)):
            within(t + lag - 5, self.units, stage)


def whole(n):
    return slice(0, n)


THIRDS = tuple((slice(a, b), whole(LANES)) for a, b in ((0, 32), (32, 48), (48, 80)))
DOWN = Sum("low_", 1, 56, D // 2, tuple((whole(56), slice(a, b)) for a, b in ((0, 256), (256, 384), (384, 640))))


def gate_up_sum(name, units, owns=1):
    return Sum(name, units, ROWS // 2, LANES, THIRDS, owns)


class GateUp:
    @staticmethod
    def scratch():
        pieces = (RING, RING, RING, ROWS // 2, LANES)
        return dict(t=pltpu.VMEM((RING, CORES, ROWS, N), f32), oh=pltpu.VMEM(pieces, f32), sb=pltpu.VMEM(pieces, bf16), halfsem=sem())

    def __init__(self, place, refs, s, come):
        self.place, self.s, self.come = place, s, come
        self.t, self.oh, self.sb, self.sent = refs["t"], refs["oh"], refs["sb"], refs["halfsem"]

    def multiply(self, u, a, sides, free=None):
        for m, side in enumerate(sides):
            self.t[...] = lax.dot_general(a[...], side[...], ROW_BY_ROW, preferred_element_type=f32).reshape(self.t.shape)
            if not m:
                when(u > 0, arrive, self.sb, self.sent)
                if free:
                    free()

            def halve(x, m=m):
                for y in range(RING):
                    for h in range(2):
                        part = (slice(h * ROWS // 2, (h + 1) * ROWS // 2), slice(y * LANES, (y + 1) * LANES))
                        self.sb[x, y, 2 * m + h] = self.t[(x, 1 - self.place.core) + part].astype(bf16)
                        self.oh[x, y, 2 * m + h] = self.t[(x, self.place.core) + part]

            loop(RING, halve)
        send(self.sb, self.s.at[u], self.sent, self.come.at[u], self.place.partner())

    def join(self, u):
        arrive(self.s.at[u], self.come.at[u])

        def one(x):
            for y in range(RING):
                for z in range(RING):
                    t = self.oh[x, y, z] + self.s[u, x, y, z].astype(f32)
                    self.oh[x, y, z] = t
                    self.s[u, x, y, z] = t.astype(bf16)

        loop(RING, one)

    def keep(self, total, u):
        for k, (own,) in total.refs("own"):
            me = self.place.at[ORDERS[k][0]]

            def some(i, k=k, own=own, me=me):
                own[lax.rem(u, total.owns), i] = self.oh[total.piece(k, me, i, ALL) + total.cuts[k]]

            loop(RING, some)

    def finish(self):
        arrive(self.sb, self.sent)


class Down:
    PIECE = (RING, RING, DOWN.rows, DOWN.cols)

    @classmethod
    def scratch(cls):
        return dict(
            hid=pltpu.VMEM((2, T, WIDE), bf16),
            td=pltpu.VMEM((CORES, ROWS_DOWN, D), f32),
            ohd=pltpu.VMEM((2,) + cls.PIECE, f32),
            sbd=pltpu.VMEM((2,) + cls.PIECE, bf16),
            hidsem=sem(2),
            f_snd=sem(2),
        )

    def __init__(self, place, total, refs, hid, come):
        self.place, self.total, self.source, self.come = place, total, hid, come
        self.hid, self.t, self.oh, self.sb, self.sem, self.sent = (refs[n] for n in ("hid", "td", "ohd", "sbd", "hidsem", "f_snd"))

    def block(self, i):
        return self.place.along(X, i + 1)[0]

    def load(self, i):
        slot = lax.rem(i, 2)
        return pltpu.make_async_copy(self.source.at[:, at(self.block(i), WIDE)], self.hid.at[slot], self.sem.at[slot])

    def multiply(self, i, dy):
        slot = lax.rem(i, 2)
        self.load(i).wait()
        when(i + 1 < RING, lambda: self.load(i + 1).start())
        self.t[...] = lax.dot_general(self.hid[slot], dy[...], ROW_BY_ROW, preferred_element_type=f32).reshape(self.t.shape)
        when(i > 1, arrive, self.sb.at[slot], self.sent.at[slot])
        for y in range(RING):
            for z in range(RING):
                row, col = (2 * y + z // 2) * DOWN.rows, (z % 2) * DOWN.cols
                part = (slice(row, row + DOWN.rows), slice(col, col + DOWN.cols))
                self.sb[slot, y, z] = self.t[(1 - self.place.core,) + part].astype(bf16)
                self.oh[slot, y, z] = self.t[(self.place.core,) + part]
        send(self.sb.at[slot], self.total.s.at[0, self.block(i)], self.sent.at[slot], self.come.at[i], self.place.partner())

    def join(self, i):
        slot, x = lax.rem(i, 2), self.block(i)
        s = self.total.s.at[0, x]
        arrive(s, self.come.at[i])

        def one(y):
            for z in range(RING):
                t = self.oh[slot, y, z] + s[y, z].astype(f32)
                self.oh[slot, y, z] = t
                s[y, z] = t.astype(bf16)

        loop(RING, one)
        (_, (p0, first)), (_, (p1, second)), (_, (p2, third)) = self.total.refs("p", "own")
        me, (cut_x, cut_y, cut_z) = self.place.at, self.total.cuts

        def pass_on(k, n, q, to):
            src, dst = ((s.at[(q, ALL) + cut_y], p1.at[0, n, x]), (s.at[(ALL, q) + cut_z], p2.at[0, n, x]))[k - 1]
            send(src, dst, self.total.sem("snd", 0, 0, k), self.total.sem("rcv", 0, 0, k), to)

        for n in OTHERS:
            for k in (1, 2):
                pass_on(k, n - 1, *self.place.along(ORDERS[k][0], n))

        def to_its_chip():
            _, to = self.place.along(X, i + 1)
            send(s.at[(ALL, ALL) + cut_x], p0.at[0, i], self.total.sem("snd", 0, 0, 0), self.total.sem("rcv", 0, 0, 0), to)

        def mine():
            for y in range(RING):
                first[0, y] = self.oh[(slot, y, ALL) + cut_x]

        when(i < RING - 1, to_its_chip)
        when(i == RING - 1, mine)
        for y in range(RING):
            second[0, x, y] = self.oh[(slot, me[Y], y) + cut_y]
            third[0, x, y] = self.oh[(slot, y, me[Z]) + cut_z]

    def run(self, dy, beside=lambda i: None):
        def step(i):
            beside(i)
            within(i, RING, lambda i: self.multiply(i, dy))
            within(i - 1, RING, self.join)

        loop(RING + 1, step)
        for slot in range(2):
            arrive(self.sb.at[slot], self.sent.at[slot])


def normed(h):
    wide = h.astype(f32)
    return (wide * lax.rsqrt(jnp.mean(wide * wide, -1, keepdims=True) + 1e-6)).astype(bf16)


def backward(by, g, u):
    by = by.astype(bf16).astype(f32)
    s = jax.nn.sigmoid(g)
    gated = g * s
    return (by * u * (s * (1.0 + g * (1.0 - s)))).astype(bf16), (by * gated).astype(bf16), (gated * u).astype(bf16)


def call(kernel, name, outs, scratch, collective_id, *args):
    anywhere = pl.BlockSpec(memory_space=pl.ANY)
    return pl.pallas_call(
        functools.partial(kernel, names=tuple(scratch)),
        out_shape=outs,
        in_specs=[anywhere] * len(args),
        out_specs=[anywhere] * len(outs),
        scratch_shapes=list(scratch.values()),
        compiler_params=pltpu.CompilerParams(collective_id=collective_id, has_side_effects=True, vmem_limit_bytes=VMEM_ALL),
        name=name,
    )(*args)


def shape(*dims, dtype=bf16):
    return jax.ShapeDtypeStruct(dims, dtype)


def named(names, scratch):
    return dict(zip(names, scratch, strict=True))


GATHERED = (CHUNKS, 2, RING, CORES, ROWS, N)


EARLY = gate_up_sum("e_", 3)
LATE = gate_up_sum("l_", CHUNKS - EARLY.units, CHUNKS - EARLY.units)


SHORT = 256
SECOND, THIRD = 11, 19


def forward_kernel(x, dy_in, w_gate, w_up, w_down, a_out, hid_out, gu_out, w_out, d_out, h_out, hid1_out, dg_out, du_out, ga_out, s_out, oh_out, *scratch, names):
    refs = named(names, scratch)
    blocks, low, a, lsem = (refs[n] for n in ("blocks", "low", "a", "lsem"))
    pairs = [(w.at[n], blocks.at[n, m]) for n in range(LAYERS) for m, w in enumerate((w_gate, w_up))] + [(w_down, low), (x, a)]
    loads = [pltpu.make_async_copy(*pair, lsem.at[n]) for n, pair in enumerate(pairs)]
    start(loads)
    place = Place()
    place.meet()
    gather = Gather(place, refs, w_out, blocks)
    down = DownGather(place, refs, d_out, low)
    wait(loads[:4])
    loop(2, gather.start_x)
    wait(loads[4:])

    def norm(i):
        a[at(i, 64)] = normed(a[at(i, 64)])

    loop(T // 64, norm)
    gather.pass_x(0)
    gather.start_x(2)

    def fetches(t):
        within(t - 1, CHUNKS, gather.start_d)
        within(t, CHUNKS, gather.start_yz)
        within(t + 1, CHUNKS, gather.pass_x)
        for stage, first, second in ((down.start_d, 6, 9), (down.start_yz, 5, 7), (down.pass_x, 4, 5), (down.start_x, 3, 3)):
            within(t - first, down.parted, stage)
            within(t - second - down.parted, down.parted, lambda u, stage=stage: stage(u + down.parted))
        within(t - THIRD + 1, CHUNKS, lambda u: gather.start_yz(u + CHUNKS))
        within(t - THIRD + 3, CHUNKS, lambda u: gather.pass_x(u + CHUNKS))
        within(t - SECOND - 1, CHUNKS, lambda u: gather.start_x(u + CHUNKS))
        within(t + 3, CHUNKS, gather.start_x)

    def load_chunk(u, wv, vsem):
        gather.ready(u)
        slot = lax.rem(u, 2)
        start(chunk_of(place, w_out.at[u // CHUNKS], lax.rem(u, CHUNKS), wv.at[slot], vsem.at[slot]))

    def layer0(wv, hs, gs, asem, vsem, hsem, gsem):
        keep = pltpu.make_async_copy(a, a_out, asem)
        keep.start()

        def outs(j, i):
            return (
                pltpu.make_async_copy(hs.at[i], hid_out.at[at(i, TILE), at(j, N)], hsem.at[i]),
                pltpu.make_async_copy(gs.at[i], gu_out.at[j, :, at(i, TILE)], gsem.at[i]),
            )

        def compute(j):
            slot = lax.rem(j, 2)
            arrive(wv.at[slot], vsem.at[slot])

            def tile(i):
                when(j > 0, lambda: wait(outs(j, i)))
                g, u = (jnp.dot(a[at(i, TILE)], wv[slot, m].reshape(D, N), preferred_element_type=f32) for m in range(2))
                gs[i, 0], gs[i, 1] = g, u
                hs[i] = (g * jax.nn.sigmoid(g) * u).astype(bf16)
                start(outs(j, i))
                when((i == 0) & (j + 1 < CHUNKS), load_chunk, j + 1, wv, vsem)

            loop(T // TILE, tile)

        def step(t):
            fetches(t)
            when(t == 1, load_chunk, 0, wv, vsem)
            within(t - 2, CHUNKS, compute)

        loop(SECOND, step)
        keep.wait()
        for i in range(T // TILE):
            wait(outs(CHUNKS - 1, i))

    pl.run_scoped(
        layer0,
        pltpu.VMEM((2,) + GATHERED[1:], bf16),
        pltpu.VMEM((T // TILE, TILE, N), bf16),
        pltpu.VMEM((T // TILE, 2, TILE, N), f32),
        *[sem()] + [sem(2)] * 3,
    )
    loop(down.parted, down.ready)

    def between(dv, hv, xv, dsem, hsem, xsem, osem):
        def loads(i, slot):
            return (
                pltpu.make_async_copy(hid_out.at[at(i, SHORT)], hv.at[slot], hsem.at[slot]),
                pltpu.make_async_copy(x.at[at(i, SHORT)], xv.at[slot], xsem.at[slot]),
            )

        def store(i, slot):
            return pltpu.make_async_copy(xv.at[slot], h_out.at[at(i, SHORT)], osem.at[slot])

        for k in range(RING):
            pltpu.make_async_copy(d_out.at[0, k], dv.at[place.along(X, k)[0]], dsem).start()
        start(loads(0, 0))
        arrive(dv, dsem)

        def step(i):
            fetches(i + SECOND)
            slot = lax.rem(i, 2)
            wait(loads(i, slot))
            when(i > 0, lambda: store(i, 1 - slot).wait())
            when(i + 1 < T // SHORT, lambda: start(loads(i + 1, 1 - slot)))
            h = xv[slot] + jnp.dot(hv[slot], dv[...].reshape(F, D), preferred_element_type=f32).astype(bf16)
            xv[slot] = h
            a[at(i, SHORT)] = normed(h)
            store(i, slot).start()

        loop(T // SHORT, step)
        store(0, 1).wait()

    pl.run_scoped(
        between,
        pltpu.VMEM((RING, CORES, ROWS_DOWN, D), bf16),
        pltpu.VMEM((2, SHORT, F), bf16),
        pltpu.VMEM((2, SHORT, D), bf16),
        sem(),
        *[sem(2)] * 3,
    )
    loop(down.parted, lambda u: down.ready(u + down.parted))
    s = refs["s"]
    total = EARLY.bind(place, refs, s)

    def layer1(dy, dv, wv, side, ysem, dsem, vsem, osem, ksem, **refs_grads):
        grads = GateUp(place, refs_grads, s, refs["come"])
        load = pltpu.make_async_copy(dy_in, dy, ysem)
        load.start()

        def fetch(j):
            slot = lax.rem(j, 2)
            start(hidden_rows(place, d_out.at[1].reshape(RING, WIDE, D), j, dv.at[slot], dsem.at[slot]))
            load_chunk(j + CHUNKS, wv, vsem)

        def outs(j):
            return [pltpu.make_async_copy(side.at[n], out.at[:, at(j, N)], osem.at[n]) for n, out in enumerate((dg_out, du_out, hid1_out))]

        def leave(u):
            late = u - EARLY.units
            return (pltpu.make_async_copy(s.at[u], s_out.at[late], ksem.at[0]), pltpu.make_async_copy(grads.oh, oh_out.at[late], ksem.at[1]))

        def join(u):
            grads.join(u)

            def go_on():
                grads.keep(total, u)
                total.start1(u)

            when(u < EARLY.units, go_on)
            when(u >= EARLY.units, lambda: start(leave(u)))

        gather.start_d(CHUNKS)
        fetch(0)
        load.wait()

        def step(j):
            fetches(j + THIRD)
            slot = lax.rem(j, 2)
            arrive(dv.at[slot], dsem.at[slot])
            arrive(wv.at[lax.rem(j + CHUNKS, 2)], vsem.at[lax.rem(j + CHUNKS, 2)])
            when(j > 0, lambda: wait(outs(j)))

            def tile(i):
                rows = at(i, TILE)
                g, u = (jnp.dot(a[rows], wv[lax.rem(j + CHUNKS, 2), m].reshape(D, N), preferred_element_type=f32) for m in range(2))
                by = lax.dot_general(dy[rows], dv[slot], BY_LAST, preferred_element_type=f32)
                side[0, rows], side[1, rows], side[2, rows] = backward(by, g, u)

            loop(T // TILE, tile)
            start(outs(j))
            within(j + 1, CHUNKS, lambda j: gather.start_d(j + CHUNKS))
            total.stages(j - 1)
            within(j - 1, CHUNKS, join)

            def halfway():
                when(j > EARLY.units, lambda: wait(leave(j - 1)))
                within(j + 1, CHUNKS, fetch)

            grads.multiply(j, a, (side.at[0], side.at[1]), halfway)

        loop(CHUNKS, step)
        total.stages(CHUNKS - 1)
        join(CHUNKS - 1)
        total.stages(CHUNKS)
        wait(leave(CHUNKS - 1))
        grads.finish()
        wait(outs(CHUNKS - 1))

    pl.run_scoped(
        layer1,
        pltpu.VMEM((T, D), bf16),
        pltpu.VMEM((2, N, D), bf16),
        pltpu.VMEM((2,) + GATHERED[1:], bf16),
        pltpu.VMEM((3, T, N), bf16),
        *[sem()] + [sem(2)] * 2 + [sem(3), sem(2)],
        **GateUp.scratch(),
    )
    keep = pltpu.make_async_copy(total.ga, ga_out, lsem.at[0])
    keep.start()
    gather.finish()
    down.finish()
    total.finish()
    keep.wait()


def forward(x, dy, w_gate, w_up, w_down, collective_id):
    pieces = (RING, RING, RING, ROWS // 2, LANES)
    early = EARLY.scratch()
    del early["e_s"]
    scratch = dict(
        Gather.scratch(),
        **DownGather.scratch(),
        **early,
        s=pltpu.VMEM((CHUNKS,) + pieces, bf16),
        come=sem(CHUNKS),
        a=pltpu.VMEM((T, D), bf16),
        blocks=pltpu.VMEM((LAYERS, 2, ROWS, F), bf16),
        low=pltpu.VMEM((LAYERS, ROWS_DOWN, D), bf16),
        lsem=sem(6),
    )
    outs = [shape(T, D), shape(T, F), shape(CHUNKS, 2, T, N, dtype=f32), shape(LAYERS, *GATHERED), shape(LAYERS, RING, CORES, ROWS_DOWN, D)]
    outs += [shape(T, D)] + [shape(T, F)] * 3 + [shape(EARLY.units, RING, RING, ROWS // 2, LANES)]
    outs += [shape(LATE.units, *pieces), shape(LATE.units, *pieces, dtype=f32)]
    return call(forward_kernel, "forward", outs, scratch, collective_id, x, dy, w_gate, w_up, w_down)


TALL_TILE = 512


def fourth_kernel(hid, dy_in, dg, du, w, h, s_in, oh_in, dh_out, ga_out, gd_out, *scratch, names):
    refs = named(names, scratch)
    dy, lsem, csem, osem = (refs[n] for n in ("dy", "lsem", "csem", "osem"))
    load = pltpu.make_async_copy(dy_in, dy, lsem)
    load.start()
    place = Place()
    late, low = LATE.bind(place, refs), DOWN.bind(place, refs)
    carried = [pltpu.make_async_copy(s_in, late.s, csem.at[3])]
    for k, (own,) in late.refs("own"):
        pieces = (ALL,) + late.piece(k, place.at[ORDERS[k][0]]) + late.cuts[k]
        carried.append(pltpu.make_async_copy(oh_in.at[pieces], own, csem.at[k]))
    start(carried)
    place.meet()
    wait(carried)

    def late_stages(t):
        late.stages(t)
        within(t + 1, late.units, late.start1)

    loop(2, late.start1)

    def multiply_down(**refs_down):
        down = Down(place, low, refs_down, hid, refs["come"])
        down.load(0).start()
        load.wait()
        down.run(dy)

    pl.run_scoped(multiply_down, **Down.scratch())

    def multiply_back(gv, wv, acc, hv, gsem, hsem):
        def loads(j, slot):
            for n, side in enumerate((dg, du)):
                yield pltpu.make_async_copy(side.at[:, at(j, N)], gv.at[slot, n], gsem.at[slot, n])

        def fetch(j):
            slot = lax.rem(j, 2)
            start(loads(j, slot))
            start(chunk_of(place, w.at[1], j, wv.at[slot], gsem.at[slot, 2]))

        fetch(0)

        def step(j):
            slot = lax.rem(j, 2)
            wait(loads(j, slot))
            arrive(wv.at[slot], gsem.at[slot, 2])
            within(j + 1, CHUNKS, fetch)
            late_stages(j + 1)
            low.stages(j)

            def tile(i):
                rows = at(i, TALL_TILE)
                by, more = (lax.dot_general(gv[slot, m, rows], wv[slot, m].reshape(D, N), BY_LAST, preferred_element_type=f32) for m in range(2))
                by += more

                def first_time():
                    acc[rows] = by

                def again():
                    acc[rows] += by

                when(j == 0, first_time)
                when(j > 0, again)

            loop(T // TALL_TILE, tile)

        loop(CHUNKS, step)

        def tile_of_h(i):
            slot = lax.rem(i, 2)
            return pltpu.make_async_copy(h.at[at(i, 256)], hv.at[slot], hsem.at[slot])

        tile_of_h(0).start()
        late.stages(CHUNKS + 1)

        def norm(i):
            tile_of_h(i).wait()
            when(i + 1 < T // 256, lambda: tile_of_h(i + 1).start())

            def part(n):
                rows = pl.ds(pl.multiple_of(i * 256 + n * 64, 64), 64)
                wide = hv[lax.rem(i, 2), at(n, 64)].astype(f32)
                by = acc[rows].astype(bf16).astype(f32)
                scale = lax.rsqrt(jnp.mean(wide * wide, -1, keepdims=True) + 1e-6)
                along = jnp.mean(by * wide, -1, keepdims=True)
                dy[rows] = dy[rows] + (by * scale - wide * (scale * scale * scale * along)).astype(bf16)

            loop(4, part)

        loop(T // 256, norm)

    pl.run_scoped(
        multiply_back,
        pltpu.VMEM((2, 2, T, N), bf16),
        pltpu.VMEM((2,) + GATHERED[1:], bf16),
        pltpu.VMEM((T, D), f32),
        pltpu.VMEM((2, 256, D), bf16),
        sem(2, 3),
        sem(2),
    )
    results = [pltpu.make_async_copy(v, out, osem.at[n]) for n, (v, out) in enumerate(((dy, dh_out), (late.ga, ga_out), (low.ga.at[0], gd_out)))]
    start(results)
    late.finish()
    low.finish()
    wait(results)


def fourth(hid, dy, dg, du, w, h, s, oh, collective_id):
    scratch = dict(
        LATE.scratch(),
        **DOWN.scratch(),
        come=sem(RING),
        dy=pltpu.VMEM((T, D), bf16),
        lsem=sem(),
        csem=sem(4),
        osem=sem(3),
    )
    outs = [shape(T, D), shape(LATE.units, RING, RING, ROWS // 2, LANES), shape(*Down.PIECE)]
    return call(fourth_kernel, "fourth", outs, scratch, collective_id, hid, dy, dg, du, w, h, s, oh)


LAST = gate_up_sum("e_", CHUNKS)


def fifth_kernel(hid, dy_in, a_in, d, gu, ga_early, ga_late, gd_in, ga_out, gd_out, sum_out, *scratch, names):
    refs = named(names, scratch)
    dy, lsem, osem = (refs[n] for n in ("dy", "lsem", "osem"))
    load = pltpu.make_async_copy(dy_in, dy, lsem)
    load.start()
    place = Place()
    others = place.shard_group()
    place.meet(others)
    total, low = LAST.bind(place, refs), DOWN.bind(place, refs)

    def multiply_down(**refs_down):
        down = Down(place, low, refs_down, hid, refs["come"])
        down.load(0).start()
        load.wait()
        down.run(dy)

    pl.run_scoped(multiply_down, **Down.scratch())
    tiles, ahead = T // TALL_TILE, 3

    def multiply_gates(a, dv, gv, side, asem, dsem, gsem, **refs_grads):
        grads = GateUp(place, refs_grads, total.s, refs["arrived"])
        load_a = pltpu.make_async_copy(a_in, a, asem)

        def rows_of_d(j):
            start(hidden_rows(place, d.at[0], j, dv, dsem))

        def tile_of_gu(n):
            slot = lax.rem(n, ahead)
            return pltpu.make_async_copy(gu.at[n // tiles, :, at(lax.rem(n, tiles), TALL_TILE)], gv.at[slot], gsem.at[slot])

        rows_of_d(0)
        start([load_a] + [tile_of_gu(n) for n in range(ahead)])

        def join(u):
            grads.join(u)
            grads.keep(total, u)
            total.start1(u)

        def back(j):
            arrive(dv, dsem)

            def tile(i):
                n = j * tiles + i
                tile_of_gu(n).wait()
                by = lax.dot_general(dy[at(i, TALL_TILE)], dv[...], BY_LAST, preferred_element_type=f32)
                side[0, at(i, TALL_TILE)], side[1, at(i, TALL_TILE)], _ = backward(by, gv[lax.rem(n, ahead), 0], gv[lax.rem(n, ahead), 1])
                when(n + ahead < CHUNKS * tiles, lambda: tile_of_gu(n + ahead).start())

            loop(tiles, tile)
            within(j + 1, CHUNKS, rows_of_d)

        def step(t):
            within(t, CHUNKS, back)
            low.stages(t)
            total.stages(t - 1)
            within(t - 1, CHUNKS, join)
            when(t == 0, load_a.wait)
            within(t, CHUNKS, lambda j: grads.multiply(j, a, (side.at[0], side.at[1])))

        loop(CHUNKS + 1, step)
        grads.finish()

    pl.run_scoped(
        multiply_gates,
        pltpu.VMEM((T, D), bf16),
        pltpu.VMEM((N, D), bf16),
        pltpu.VMEM((ahead, 2, TALL_TILE, N), f32),
        pltpu.VMEM((2, T, N), bf16),
        sem(),
        sem(),
        sem(ahead),
        **GateUp.scratch(),
    )

    def square(g, d, gsem):
        loads = [pltpu.make_async_copy(*pair, gsem.at[n]) for n, pair in enumerate(((ga_early, g.at[:EARLY.units]), (ga_late, g.at[EARLY.units :]), (gd_in, d)))]
        start(loads)
        total.stages(CHUNKS)
        squares = refs["squares"]
        me = place.at[X] * CORES + place.core
        mine = squares.at[me]
        mine[...] = jnp.zeros(mine.shape, f32)

        def add(piece):
            for n in range(0, piece.shape[1], LANES):
                t = piece[:, n : n + LANES].astype(f32)
                mine[...] += jnp.sum((t * t).reshape((-1,) + mine.shape), 0)

        def add_all(all_gates, all_down):
            loop(CHUNKS * RING, lambda i: [add(all_gates[i // RING, lax.rem(i, RING), z]) for z in range(RING)])
            loop(RING, lambda y: [add(all_down[y, z]) for z in range(RING)])

        wait(loads)
        add_all(g, d)
        loop(4, lambda t: total.stages(t + CHUNKS + 1))
        add_all(total.ga, low.ga.at[0])
        for to in others + [place.partner()] + [place.along(X, k)[1] for k in OTHERS]:
            send(mine, mine, refs["q_snd"], refs["q_rcv"], to)
        for semaphore in (refs["q_rcv"], refs["q_snd"]):
            arrive(squares.at[: BLOCKS - 1], semaphore)
        sum_ref = refs["sum"]
        sum_ref[...] = squares[0]
        for n in range(1, BLOCKS):
            sum_ref[...] += squares[n]

    pl.run_scoped(square, pltpu.VMEM(total.ga.shape, bf16), pltpu.VMEM(Down.PIECE, bf16), sem(3))
    results = [pltpu.make_async_copy(v, out, osem.at[n]) for n, (v, out) in enumerate(((total.ga, ga_out), (low.ga.at[0], gd_out), (refs["sum"], sum_out)))]
    start(results)
    total.finish()
    low.finish()
    wait(results)


def fifth(hid, dy, a, d, gu, *layer1, collective_id):
    scratch = dict(
        LAST.scratch(),
        **DOWN.scratch(),
        come=sem(RING),
        arrived=sem(CHUNKS),
        dy=pltpu.VMEM((T, D), bf16),
        lsem=sem(),
        osem=sem(3),
        squares=pltpu.VMEM((BLOCKS, 8, LANES), f32),
        sum=pltpu.VMEM((8, LANES), f32),
        q_snd=sem(),
        q_rcv=sem(),
    )
    outs = [shape(CHUNKS, RING, RING, ROWS // 2, LANES), shape(*Down.PIECE), shape(8, LANES, dtype=f32)]
    return call(fifth_kernel, "fifth", outs, scratch, collective_id, hid, dy, a, d.reshape(LAYERS, RING, WIDE, D), gu, *layer1)


SLOTS = 4
TALL = 2 * 2 * DOWN.rows


def sixth_kernel(*args, names):
    (total, *gradients), args = args[:6], args[6:]
    weights, outs, refs = args[:9], args[9:18], named(names, args[18:])
    g1, g0, d1, d0, sv = (refs[n] for n in ("g1", "g0", "d1", "d0", "sv"))
    early, late, down1, both0, down0 = gradients
    pairs = ((total, sv), (early, g1.at[: EARLY.units]), (late, g1.at[EARLY.units :]), (both0, g0), (down1, d1), (down0, d0))
    loads = [pltpu.make_async_copy(*pair, refs["lsem"].at[n]) for n, pair in enumerate(pairs)]
    start(loads)

    def copies(n, arrays, into, which, kind):
        per, rows, buffers = (RING, ROWS // 2, ("gw", "gm", "gv")) if kind < 2 else (2, TALL, ("dw", "dm", "dv"))
        slot = lax.rem(n, SLOTS)
        for i, buffer in enumerate(buffers):
            there, here = arrays[3 * i + kind].at[n // per, at(lax.rem(n, 2), rows)], refs[buffer].at[slot]
            yield pltpu.make_async_copy(*((there, here) if into else (here, there)), refs["sems"].at[which, kind // 2, slot, i])

    def gates(n, do, arrays, into, which):
        for kind in range(2):
            when(lax.rem(n, RING) // 2 == kind, lambda kind=kind: do(copies(n, arrays, into, which, kind)))

    def downs(n, do, arrays, into, which):
        do(copies(n, arrays, into, which, 2))

    wait(loads[:1])
    squares = jnp.sum(sv[...], keepdims=True)
    factor = jnp.minimum(1.0, 0.5 * lax.rsqrt(squares / (LAYERS * 3 * D * F) + 1e-30))

    def adamw(slot, buffers, part, g):
        w, m, v = (refs[b].at[slot] for b in buffers)
        g = g.astype(f32) * factor
        new_m = 0.9 * m[part] + 0.1 * g
        new_v = 0.95 * v[part] + 0.05 * g * g
        old = w[part].astype(f32)
        w[part] = (old - 0.02 * (new_m * lax.rsqrt(new_v + 1e-8) + 0.1 * old)).astype(bf16)
        m[part], v[part] = new_m, new_v

    def begin(transfer):
        loop(SLOTS - 1, lambda n: transfer(n, start, weights, True, 0))

    def run(steps, transfer, body):
        def step(n):
            transfer(n, wait, weights, True, 0)
            body(n, lax.rem(n, SLOTS))
            transfer(n, start, outs, False, 1)
            when(n > 0, lambda: transfer(n - 1, wait, outs, False, 1))
            within(n + SLOTS - 1, steps, lambda n: transfer(n, start, weights, True, 0))

        loop(steps, step)
        transfer(jnp.int32(steps - 1), wait, outs, False, 1)

    def gate_step(n, slot):
        def of(g):
            def chunk(j):
                for y in range(RING):
                    adamw(slot, ("gw", "gm", "gv"), (ALL, at(j * RING + y, LANES)), g[j, y, lax.rem(n, RING)])

            loop(CHUNKS, chunk)

        when(n < RING, of, g0)
        when(n >= RING, of, g1)

    def down_step(n, slot):
        def of(d):
            for y in range(2):
                for z in range(RING):
                    row, col = (2 * y + z // 2) * DOWN.rows, (z % 2) * DOWN.cols
                    part = (slice(row, row + DOWN.rows), slice(col, col + DOWN.cols))
                    adamw(slot, ("dw", "dm", "dv"), part, d[2 * lax.rem(n, 2) + y, z])

        when(n < 2, of, d0)
        when(n >= 2, of, d1)

    begin(gates)
    begin(downs)
    wait(loads[1:])
    run(LAYERS * RING, gates, gate_step)
    run(LAYERS * 2, downs, down_step)


def sixth(total, gradients, weights):
    half, tall = (SLOTS, ROWS // 2, F), (SLOTS, TALL, D)
    pieces = pltpu.VMEM((CHUNKS, RING, RING, ROWS // 2, LANES), bf16)
    scratch = dict(g1=pieces, g0=pieces, d1=pltpu.VMEM(Down.PIECE, bf16), d0=pltpu.VMEM(Down.PIECE, bf16), sv=pltpu.VMEM((8, LANES), f32))
    for name, dims in (("g", half), ("d", tall)):
        scratch.update({name + "w": pltpu.VMEM(dims, bf16), name + "m": pltpu.VMEM(dims, f32), name + "v": pltpu.VMEM(dims, f32)})
    scratch.update(lsem=sem(6), sems=sem(2, 2, SLOTS, 3))
    outs = [shape(*w.shape, dtype=w.dtype) for w in weights]
    return call(sixth_kernel, "sixth", outs, scratch, None, total, *gradients, *weights)


def solution(mesh):
    def step(x, dy, *arrays):
        w_gate, w_up, w_down = arrays[:3]
        x, dy = x[0], dy[0]
        a0, hid0, gu0, w, d, h1, hid1, dg1, du1, early, s, oh = forward(x, dy, w_gate, w_up, w_down, 0)
        dh1, late, down1 = fourth(hid1, dy, dg1, du1, w, h1, s, oh, 1)
        both0, down0, total = fifth(hid0, dh1, a0, d, gu0, early, late, down1, collective_id=2)
        return tuple(sixth(total, (early, late, down1, both0, down0), arrays))

    states, cut = P(("rep", "r", "s"), None, None), P(None, "s", None)
    return jax.shard_map(
        step,
        mesh=mesh,
        in_specs=(states, states) + (cut,) * 9,
        out_specs=(P("rep", "s", None),) * 9,
        check_vma=False,
    )
```
